32 devices in a mesh: dp: 1 (over z), sp: 4 (over y), tp: 8 (over x, core).
Axes of the slice: x: 4, y: 4, z: 1, core: 2. Of those that a mesh axis runs over, the one named last changes fastest.
The devices are a block of a 4x4x8 slice.
Arguments:
- x: bfloat16 [8192, 2560], P(('dp', 'sp', 'tp'))
- segment_ids: int32 [8192], P(('dp', 'sp', 'tp'))
- positions: int32 [8192], P(('dp', 'sp', 'tp'))
- g_attn: bfloat16 [2, 2560], replicated
- w_q: bfloat16 [2, 2560, 8, 256], P(None, None, 'tp')
- w_k: bfloat16 [2, 2560, 4, 256], replicated
- w_v: bfloat16 [2, 2560, 4, 256], replicated
- w_o: bfloat16 [2, 8, 256, 2560], P(None, 'tp')
- g_mlp: bfloat16 [2, 2560], replicated
- w_gate: bfloat16 [2, 2560, 10240], P(None, None, 'tp')
- w_up: bfloat16 [2, 2560, 10240], P(None, None, 'tp')
- w_down: bfloat16 [2, 10240, 2560], P(None, 'tp')
Outputs:
- output: bfloat16 [8192, 2560], P(('dp', 'sp', 'tp'))
All inputs are finite; a program needn't handle non-finite values.
Results may differ from the reference program's by a relative error of at most 0.0197739.
Values are sent between devices in bfloat16 or wider.
A program may use at most 768 MiB of HBM per device.

```python
import jax
import jax.numpy as jnp
from jax import lax

D = 2560
HEADS = 8
KV_HEADS = 4
HEAD = 256
FF = 10240
LAYERS = 2
TOKENS = 8192
WINDOW = 1024
ROPE_BASE = 10000
EPS = 1e-6
REF_ROWS = max(1024 // HEADS, 8)
GROUP = HEADS // KV_HEADS


def draw_layout(layout_key):
    k_first, k_second, k_step, k_offset = jax.random.split(layout_key, 4)
    first_cut = jax.random.randint(k_first, (), TOKENS // 2, 3 * TOKENS // 4)
    second_cut = jax.random.randint(k_second, (), first_cut + TOKENS // 16, TOKENS - TOKENS // 16 + 1)
    tok_index = jnp.arange(TOKENS)
    segment_ids = (tok_index >= first_cut).astype(jnp.int32) + (tok_index >= second_cut).astype(jnp.int32)
    step_sizes = jax.random.randint(k_step, (TOKENS,), 1, 8)
    before = jnp.cumsum(step_sizes) - step_sizes
    seg_starts = before[jnp.stack([jnp.zeros((), first_cut.dtype), first_cut, second_cut])]
    seg_offsets = jax.random.randint(k_offset, (3,), 0, 512)
    positions = before - seg_starts[segment_ids] + seg_offsets[segment_ids]
    return segment_ids, positions.astype(jnp.int32)


def draw_stack(stack_key, shape, scale):
    layer_keys = jax.random.split(stack_key, LAYERS)
    return lax.map(lambda one_key: (jax.random.normal(one_key, shape, jnp.float32) * scale).astype(jnp.bfloat16), layer_keys)


def setup_inputs(seed: int = 0, part: int = 0) -> dict:
    root_key = jax.random.key(seed)
    part_key = jax.random.fold_in(root_key, part)
    k_layout, k_noise, k_walk = jax.random.split(part_key, 3)
    segment_ids, positions = draw_layout(k_layout)
    noise = jax.random.normal(k_noise, (TOKENS, D), jnp.float32)
    walk = jnp.cumsum(jax.random.normal(k_walk, (TOKENS, D), jnp.float32), axis=0) * (1.5 / TOKENS ** 0.5)
    x = (0.6 * noise + walk).astype(jnp.bfloat16)
    w_keys = jax.random.split(jax.random.key(seed + 1), 8)
    gains = 1.0 + 0.5 * jax.random.normal(w_keys[0], (2, LAYERS, D), jnp.float32)
    return {
        "x": x,
        "segment_ids": segment_ids,
        "positions": positions,
        "g_attn": gains[0].astype(jnp.bfloat16),
        "w_q": draw_stack(w_keys[1], (D, HEADS, HEAD), D ** -0.5),
        "w_k": draw_stack(w_keys[2], (D, KV_HEADS, HEAD), D ** -0.5),
        "w_v": draw_stack(w_keys[3], (D, KV_HEADS, HEAD), D ** -0.5),
        "w_o": draw_stack(w_keys[4], (HEADS, HEAD, D), (HEADS * HEAD) ** -0.5),
        "g_mlp": gains[1].astype(jnp.bfloat16),
        "w_gate": draw_stack(w_keys[5], (D, FF), D ** -0.5),
        "w_up": draw_stack(w_keys[6], (D, FF), D ** -0.5),
        "w_down": draw_stack(w_keys[7], (FF, D), FF ** -0.5),
    }


def rms_norm(x, gain):
    x_wide = x.astype(jnp.float32)
    inv_rms = lax.rsqrt(jnp.mean(x_wide * x_wide, axis=-1, keepdims=True) + EPS)
    return (x_wide * inv_rms * gain.astype(jnp.float32)).astype(jnp.bfloat16)


def rope(t, cos_tab, sin_tab):
    half_width = HEAD // 2
    t_wide = t.astype(jnp.float32)
    lower_half = t_wide[..., :half_width]
    upper_half = t_wide[..., half_width:]
    return jnp.concatenate([lower_half * cos_tab - upper_half * sin_tab, upper_half * cos_tab + lower_half * sin_tab], axis=-1).astype(jnp.bfloat16)


def attention(q, k, v, segment_ids, windowed):
    block_rows = REF_ROWS
    key_span = min(block_rows + WINDOW, TOKENS) if windowed else TOKENS
    blocks = TOKENS // block_rows
    q_blocks = q.reshape(blocks, block_rows, KV_HEADS, GROUP, HEAD)

    def one_block(block_args):
        q_blk, block_idx = block_args
        q_start = block_idx * block_rows
        k_start = jnp.clip(q_start + block_rows - key_span, 0, TOKENS - key_span)
        k_blk = lax.dynamic_slice_in_dim(k, k_start, key_span, 0)
        v_blk = lax.dynamic_slice_in_dim(v, k_start, key_span, 0)
        seg_q = lax.dynamic_slice_in_dim(segment_ids, q_start, block_rows, 0)
        seg_k = lax.dynamic_slice_in_dim(segment_ids, k_start, key_span, 0)
        q_pos = q_start + jnp.arange(block_rows)
        k_pos = k_start + jnp.arange(key_span)
        allowed = (k_pos[None, :] <= q_pos[:, None]) & (seg_k[None, :] == seg_q[:, None])
        if windowed:
            allowed = allowed & (q_pos[:, None] - k_pos[None, :] < WINDOW)
        scores = jnp.einsum("qgrd,kgd->qgrk", q_blk.astype(jnp.float32), k_blk.astype(jnp.float32)) * HEAD ** -0.5
        scores = jnp.where(allowed[:, None, None, :], scores, -1e30)
        attn_probs = jax.nn.softmax(scores, axis=-1).astype(jnp.bfloat16).astype(jnp.float32)
        mixed = jnp.einsum("qgrk,kgd->qgrd", attn_probs, v_blk.astype(jnp.float32))
        return mixed.astype(jnp.bfloat16)

    out_blocks = lax.map(one_block, (q_blocks, jnp.arange(blocks)))
    return out_blocks.reshape(TOKENS, HEADS * HEAD)


def decoder_layer(x, params, cos_tab, sin_tab, segment_ids, windowed):
    g_attn, w_q, w_k, w_v, w_o, g_mlp, w_gate, w_up, w_down = params
    normed = rms_norm(x, g_attn)
    q = jnp.dot(normed, w_q.reshape(D, HEADS * HEAD), preferred_element_type=jnp.float32).astype(jnp.bfloat16)
    k = jnp.dot(normed, w_k.reshape(D, KV_HEADS * HEAD), preferred_element_type=jnp.float32).astype(jnp.bfloat16)
    v = jnp.dot(normed, w_v.reshape(D, KV_HEADS * HEAD), preferred_element_type=jnp.float32).astype(jnp.bfloat16)
    q = rope(q.reshape(TOKENS, HEADS, HEAD), cos_tab, sin_tab).reshape(TOKENS, KV_HEADS, GROUP, HEAD)
    k = rope(k.reshape(TOKENS, KV_HEADS, HEAD), cos_tab, sin_tab)
    v = v.reshape(TOKENS, KV_HEADS, HEAD)
    mixed = attention(q, k, v, segment_ids, windowed)
    attn_out = jnp.dot(mixed, w_o.reshape(HEADS * HEAD, D), preferred_element_type=jnp.float32).astype(jnp.bfloat16)
    hidden = (x.astype(jnp.float32) + attn_out.astype(jnp.float32)).astype(jnp.bfloat16)
    normed = rms_norm(hidden, g_mlp)
    gate_proj = jnp.dot(normed, w_gate, preferred_element_type=jnp.float32)
    up_proj = jnp.dot(normed, w_up, preferred_element_type=jnp.float32)
    activation = (jax.nn.silu(gate_proj) * up_proj).astype(jnp.bfloat16)
    mlp_out = jnp.dot(activation, w_down, preferred_element_type=jnp.float32).astype(jnp.bfloat16)
    return (hidden.astype(jnp.float32) + mlp_out.astype(jnp.float32)).astype(jnp.bfloat16)


def reference(x, segment_ids, positions, g_attn, w_q, w_k, w_v, w_o, g_mlp, w_gate, w_up, w_down):
    inv_freq = ROPE_BASE ** (-jnp.arange(HEAD // 2, dtype=jnp.float32) / (HEAD // 2))
    angles = positions.astype(jnp.float32)[:, None] * inv_freq[None, :]
    cos_tab = jnp.cos(angles)[:, None, :]
    sin_tab = jnp.sin(angles)[:, None, :]
    stacked = tuple(w.reshape((LAYERS // 2, 2) + w.shape[1:]) for w in (g_attn, w_q, w_k, w_v, w_o, g_mlp, w_gate, w_up, w_down))

    def pair_step(residual, layer_pair):
        residual = decoder_layer(residual, tuple(w[0] for w in layer_pair), cos_tab, sin_tab, segment_ids, True)
        residual = decoder_layer(residual, tuple(w[1] for w in layer_pair), cos_tab, sin_tab, segment_ids, False)
        return residual, None

    final_x, unused_ys = lax.scan(pair_step, x, stacked)
    return final_x
```

```python
import functools
import math

import jax
import jax.numpy as jnp
from jax import lax
from jax.experimental import pallas as pl
from jax.experimental.pallas import tpu as pltpu
from jax.sharding import PartitionSpec as P

EPS = 1e-6
ROPE_BASE = 10000.0
WINDOW = 1024
CHIPS = 4
MESH = pl.DeviceIdType.MESH
BF16 = jnp.bfloat16
F32 = jnp.float32
VMEM_LIMIT = 66_000_000
Q_BLOCK = 512
K_BLOCK = 512


def _place():
    t = lax.axis_index("tp")
    c = lax.rem(t, 2)
    x = t // 2
    right = lax.rem(x + 1, CHIPS) * 2 + c
    left = lax.rem(x + CHIPS - 1, CHIPS) * 2 + c
    sib = x * 2 + 1 - c
    return x, c, right, left, sib


def _copy(src, dst, sems, index, axis, dev):
    send, recv = sems
    return pltpu.make_async_remote_copy(
        src_ref=src, dst_ref=dst, send_sem=send.at[index], recv_sem=recv.at[index],
        device_id={axis: dev}, device_id_type=MESH)


def _barrier(peers):
    bar = pltpu.get_barrier_semaphore()
    for axis, dev in peers:
        pl.semaphore_signal(bar, inc=1, device_id={axis: dev}, device_id_type=MESH)
    pl.semaphore_wait(bar, len(peers))


def _piece_rows(x, c, rows, k, j):
    half = rows // 2
    core = c if j < 2 else 1 - c
    even = j % 2 == 0
    if k == 0:
        chip, h = x, j % 2
    elif k == 1:
        chip, h = (x + CHIPS - 1, 0) if even else (x + 1, 1)
    elif k == 2:
        chip, h = (x + CHIPS - 1, 1) if even else (x + 1, 0)
    else:
        chip, h = x + 2, j % 2
    return lax.rem(chip, CHIPS) * (2 * rows) + core * rows + h * half


def _gather_copies(buf, sems, rows, right, left, sib):
    half = rows // 2
    a, b = pl.ds(0, half), pl.ds(half, half)
    ring = [
        _copy(buf.at[0, a], buf.at[1, a], sems, 0, "tp", right),
        _copy(buf.at[0, b], buf.at[1, b], sems, 1, "tp", left),
        _copy(buf.at[0, b], buf.at[2, a], sems, 2, "tp", right),
        _copy(buf.at[0, a], buf.at[2, b], sems, 3, "tp", left),
        _copy(buf.at[1, a], buf.at[3, a], sems, 4, "tp", right),
        _copy(buf.at[1, b], buf.at[3, b], sems, 5, "tp", left),
    ]
    relay = [_copy(buf.at[k, pl.ds(0, rows)], buf.at[k, pl.ds(rows, rows)], sems, 6 + k, "tp", sib) for k in range(4)]
    return ring, relay


def _gather_begin(ring, relay):
    for i in (0, 1):
        ring[i].start()
    relay[0].start()
    for i in (2, 3):
        ring[i].start()


def _gather_arrive(ring, relay, k):
    if k == 1:
        ring[0].wait_recv()
        ring[4].start()
        ring[1].wait_recv()
        ring[5].start()
    elif k >= 2:
        ring[2 * k - 2].wait_recv()
        ring[2 * k - 1].wait_recv()
    if k >= 1:
        relay[k].start()
    relay[k].wait_recv()


def _gather_end(ring, relay):
    for copy in ring + relay:
        copy.wait_send()


def _norm_into(dst, x_ref, g_ref):
    rows = x_ref.shape[0]
    gain = g_ref[...].astype(F32)
    chunk = 16

    def body(i, carry):
        rs = pl.ds(pl.multiple_of(i * chunk, chunk), chunk)
        wide = x_ref[rs, :].astype(F32)
        inv = lax.rsqrt(jnp.mean(wide * wide, axis=-1, keepdims=True) + EPS)
        dst[0, rs, :] = (wide * inv * gain).astype(BF16)
        return carry

    lax.fori_loop(0, rows // chunk, body, 0)


def _add_rows(rows, body):
    chunk = 16

    def step(i, carry):
        body(pl.ds(pl.multiple_of(i * chunk, chunk), chunk))
        return carry

    lax.fori_loop(0, rows // chunk, step, 0)


class _Scatter:
    def __init__(self, part, from_sib, direct, chain, last, sems, rows, right, left, sib):
        half = rows // 2
        a, b = pl.ds(0, half), pl.ds(half, half)
        self.rows, self.part, self.from_sib = rows, part, from_sib
        self.direct, self.chain, self.last = direct, chain, last
        self.swap = [_copy(part.at[k, pl.ds(rows, rows)], from_sib.at[k], sems, k, "tp", sib) for k in range(4)]
        self.d = [_copy(part.at[2, b], direct.at[a], sems, 4, "tp", right), _copy(part.at[2, a], direct.at[b], sems, 5, "tp", left)]
        self.c = [_copy(part.at[3, b], chain.at[b], sems, 6, "tp", right), _copy(part.at[3, a], chain.at[a], sems, 7, "tp", left)]
        self.l = [_copy(part.at[1, b], last.at[b], sems, 8, "tp", right), _copy(part.at[1, a], last.at[a], sems, 9, "tp", left)]

    def _fold(self, k, extra=None):
        part, from_sib = self.part, self.from_sib

        def body(rs):
            total = part[k, rs, :].astype(F32) + from_sib[k, rs, :].astype(F32)
            if extra is not None:
                total = total + extra[rs, :].astype(F32)
            part[k, rs, :] = total.astype(BF16)

        _add_rows(self.rows, body)

    def send_direct(self):
        self.swap[2].wait_recv()
        self._fold(2)
        for copy in self.d:
            copy.start()

    def send_chain(self):
        self.swap[3].wait_recv()
        self._fold(3)
        for copy in self.c:
            copy.start()

    def forward_chain(self):
        self.swap[1].wait_recv()
        for copy in self.c:
            copy.wait_recv()
        self._fold(1, self.chain)
        for copy in self.l:
            copy.start()

    def finish(self, o_ref, x_ref):
        self.swap[0].wait_recv()
        for copy in self.d + self.l:
            copy.wait_recv()
        part, from_sib, direct, last = self.part, self.from_sib, self.direct, self.last

        def body(rs):
            total = part[0, rs, :].astype(F32) + from_sib[0, rs, :].astype(F32)
            total = total + direct[rs, :].astype(F32) + last[rs, :].astype(F32)
            o_ref[rs, :] = (x_ref[rs, :].astype(F32) + total.astype(BF16).astype(F32)).astype(BF16)

        _add_rows(self.rows, body)
        for copy in self.swap + self.d + self.c + self.l:
            copy.wait_send()


def _scatter_scratch(rows, model):
    return [
        pltpu.VMEM((4, 2 * rows, model), BF16),
        pltpu.VMEM((4, rows, model), BF16),
        pltpu.VMEM((rows, model), BF16),
        pltpu.VMEM((rows, model), BF16),
        pltpu.VMEM((rows, model), BF16),
        pltpu.SemaphoreType.DMA((10,)),
        pltpu.SemaphoreType.DMA((10,)),
    ]


def _params(collective_id):
    return pltpu.CompilerParams(collective_id=collective_id, has_side_effects=True, vmem_limit_bytes=VMEM_LIMIT)


def _mlp_kernel(layer, x_ref, g_ref, wg_hbm, wu_hbm, wd_hbm, o_ref, buf, wg, wu, wd, act, part, from_sib, direct, chain, last,
                s_send, s_recv, g_send, g_recv, w_sem):
    rows, model = x_ref.shape
    cols = wg.shape[1]
    x, c, right, left, sib = _place()
    loads = [pltpu.make_async_copy(src.at[layer], dst, w_sem.at[i]) for i, (src, dst) in enumerate(((wg_hbm, wg), (wu_hbm, wu), (wd_hbm, wd)))]
    for load in loads:
        load.start()
    _norm_into(buf, x_ref, g_ref)
    _barrier((("tp", left), ("tp", right), ("tp", sib)))
    ring, relay = _gather_copies(buf, (g_send, g_recv), rows, right, left, sib)
    _gather_begin(ring, relay)
    scatter = _Scatter(part, from_sib, direct, chain, last, (s_send, s_recv), rows, right, left, sib)
    nt = 256

    def step(k, carry):
        for kk in range(4):
            @pl.when(k == kk)
            def _():
                _gather_arrive(ring, relay, kk)
                if kk == 0:
                    loads[0].wait()
                    loads[1].wait()

        def up(n, inner):
            cs = pl.ds(pl.multiple_of(n * nt, nt), nt)
            gate = jnp.dot(buf[k], wg[:, cs], preferred_element_type=F32)
            lin = jnp.dot(buf[k], wu[:, cs], preferred_element_type=F32)
            act[:, cs] = (jax.nn.silu(gate) * lin).astype(BF16)
            return inner

        lax.fori_loop(0, cols // nt, up, 0)

        @pl.when(k == 0)
        def _():
            loads[2].wait()

        def down(n, inner):
            cs = pl.ds(pl.multiple_of(n * nt, nt), nt)
            part[k, :, cs] = jnp.dot(act[...], wd[:, cs], preferred_element_type=F32).astype(BF16)
            return inner

        lax.fori_loop(0, model // nt, down, 0)
        for kk in range(4):
            @pl.when(k == kk)
            def _():
                scatter.swap[kk].start()
                if kk == 2:
                    scatter.send_direct()
                if kk == 3:
                    scatter.send_chain()
        return carry

    lax.fori_loop(0, 4, step, 0)
    scatter.forward_chain()
    scatter.finish(o_ref, x_ref)
    _gather_end(ring, relay)


def _mlp(layer, x, gain, w_gate, w_up, w_down):
    rows, model = x.shape
    cols = w_gate.shape[2]
    vmem, hbm = pl.BlockSpec(memory_space=pltpu.VMEM), pl.BlockSpec(memory_space=pl.ANY)
    return pl.pallas_call(
        functools.partial(_mlp_kernel, layer),
        name=f"mlp_{layer}",
        out_shape=jax.ShapeDtypeStruct((rows, model), BF16),
        in_specs=[vmem, vmem, hbm, hbm, hbm],
        out_specs=vmem,
        scratch_shapes=[
            pltpu.VMEM((4, 2 * rows, model), BF16),
            pltpu.VMEM((model, cols), BF16),
            pltpu.VMEM((model, cols), BF16),
            pltpu.VMEM((cols, model), BF16),
            pltpu.VMEM((2 * rows, cols), BF16),
            *_scatter_scratch(rows, model),
            pltpu.SemaphoreType.DMA((10,)),
            pltpu.SemaphoreType.DMA((10,)),
            pltpu.SemaphoreType.DMA((3,)),
        ],
        compiler_params=_params(layer),
    )(x, gain, w_gate, w_up, w_down)


def _out_kernel(layer, m_ref, x_ref, wo_hbm, o_ref, wo, lhs, part, from_sib, direct, chain, last, s_send, s_recv, w_sem):
    rows, model = x_ref.shape
    half = rows // 2
    x, c, right, left, sib = _place()
    load = pltpu.make_async_copy(wo_hbm.at[layer], wo, w_sem.at[0])
    load.start()
    _barrier((("tp", left), ("tp", right), ("tp", sib)))
    scatter = _Scatter(part, from_sib, direct, chain, last, (s_send, s_recv), rows, right, left, sib)
    load.wait()
    nt = 512
    for k in (2, 3, 1, 0):
        for j in range(4):
            start = pl.multiple_of(_piece_rows(x, c, rows, k, j), half)
            lhs[pl.ds(j * half, half), :] = m_ref[pl.ds(start, half), :]

        def down(n, inner):
            cs = pl.ds(pl.multiple_of(n * nt, nt), nt)
            part[k, :, cs] = jnp.dot(lhs[...], wo[:, cs], preferred_element_type=F32).astype(BF16)
            return inner

        lax.fori_loop(0, model // nt, down, 0)
        scatter.swap[k].start()
        if k == 2:
            scatter.send_direct()
        if k == 3:
            scatter.send_chain()
    scatter.forward_chain()
    scatter.finish(o_ref, x_ref)


def _out_proj(layer, mixed, x, w_o):
    rows, model = x.shape
    head_dim = mixed.shape[1]
    vmem, hbm = pl.BlockSpec(memory_space=pltpu.VMEM), pl.BlockSpec(memory_space=pl.ANY)
    return pl.pallas_call(
        functools.partial(_out_kernel, layer),
        name=f"out_{layer}",
        out_shape=jax.ShapeDtypeStruct((rows, model), BF16),
        in_specs=[vmem, vmem, hbm],
        out_specs=vmem,
        scratch_shapes=[
            pltpu.VMEM((head_dim, model), BF16),
            pltpu.VMEM((2 * rows, head_dim), BF16),
            *_scatter_scratch(rows, model),
            pltpu.SemaphoreType.DMA((1,)),
        ],
        compiler_params=_params(2 + layer),
    )(mixed, x, w_o)


def _qkv_kernel(layer, gather_tab, windowed, shards, x_ref, g_ref, tab_in, wq_hbm, wkv_hbm, q_out, kv_out, *rest):
    if gather_tab:
        tab_out, rest = rest[0], rest[1:]
    buf, tab, wq, wkv, qs, kv, g_send, g_recv, t_send, t_recv, y_send, y_recv, p_send, p_recv, l_sem, q_sem, w_sem = rest
    rows, model = x_ref.shape
    half, step_rows = rows // 2, 2 * rows
    shard = 4 * step_rows
    hd = wq.shape[1]
    x, c, right, left, sib = _place()
    y = lax.axis_index("sp")
    up, down = lax.rem(y + 1, shards), lax.rem(y + shards - 1, shards)
    loads = [pltpu.make_async_copy(wq_hbm.at[layer], wq, w_sem.at[0]), pltpu.make_async_copy(wkv_hbm.at[layer], wkv, w_sem.at[1])]
    for load in loads:
        load.start()
    if not gather_tab:
        tab_load = pltpu.make_async_copy(tab_in, tab, w_sem.at[2])
        tab_load.start()
    else:
        tab_load = pltpu.make_async_copy(tab_in, tab.at[0, pl.ds(0, rows)], w_sem.at[2])
        tab_load.start()
    _norm_into(buf, x_ref, g_ref)
    tab_load.wait()
    _barrier((("tp", left), ("tp", right), ("tp", sib), ("sp", up), ("sp", down)))
    ring, relay = _gather_copies(buf, (g_send, g_recv), rows, right, left, sib)
    if gather_tab:
        t_ring, t_relay = _gather_copies(tab, (t_send, t_recv), rows, right, left, sib)
        for i in (0, 1):
            t_ring[i].start()
            ring[i].start()
        t_relay[0].start()
        relay[0].start()
        for i in (2, 3):
            t_ring[i].start()
            ring[i].start()
    else:
        _gather_begin(ring, relay)

    if windowed:
        bases = (shard, 0)
    else:
        bases = tuple(lax.rem(y + d, shards) * shard for d in (0, shards - 1, 1, 2))

    def y_copies(k):
        whole, a, b = pl.ds(k * step_rows, step_rows), pl.ds(k * step_rows, rows), pl.ds(k * step_rows + rows, rows)
        sems = (y_send, y_recv)
        first = [_copy(kv.at[0, whole], kv.at[1, whole], sems, 4 * k, "sp", up)]
        second = []
        if not windowed:
            first.append(_copy(kv.at[0, whole], kv.at[2, whole], sems, 4 * k + 1, "sp", down))
            second.append(_copy(kv.at[1, a], kv.at[3, a], sems, 4 * k + 2, "sp", up))
            second.append(_copy(kv.at[2, b], kv.at[3, b], sems, 4 * k + 3, "sp", down))
        return first, second

    def place(s, k):
        for j in range(4):
            src = kv.at[s, pl.ds(k * step_rows + j * half, half)]
            start = pl.multiple_of(bases[s] + _piece_rows(x, c, rows, k, j), half)
            dst = kv_out.at[c, pl.ds(start, half)]
            pltpu.make_async_copy(src, dst, l_sem.at[s]).start()
            _copy(src, dst, (p_send, p_recv), s, "tp", sib).start()

    def forward(k):
        first, second = y_copies(k)
        for copy in first:
            copy.wait_recv()
        for copy in second:
            copy.start()
        place(1, k)
        if not windowed:
            place(2, k)

    def opposite(k):
        first, second = y_copies(k)
        for copy in second:
            copy.wait_recv()
        if second:
            place(3, k)

    def step(k, carry):
        for kk in range(4):
            @pl.when(k == kk)
            def _():
                if kk == 0:
                    loads[0].wait()
                    loads[1].wait()
                if gather_tab:
                    _gather_arrive(t_ring, t_relay, kk)
                _gather_arrive(ring, relay, kk)

        cos, sin = tab[k, :, :hd // 2], tab[k, :, hd // 2:]

        def rotate(t):
            lower, upper = t[:, :hd // 2], t[:, hd // 2:]
            return jnp.concatenate([lower * cos - upper * sin, upper * cos + lower * sin], axis=-1).astype(BF16)

        q = jnp.dot(buf[k], wq[...], preferred_element_type=F32).astype(BF16).astype(F32)
        rs = pl.ds(pl.multiple_of(k * step_rows, step_rows), step_rows)
        qs[rs, :] = rotate(q)
        t = jnp.dot(buf[k], wkv[...], preferred_element_type=F32).astype(BF16)

        @pl.when(c == 0)
        def _():
            kv[0, rs, :] = rotate(t.astype(F32))

        @pl.when(c == 1)
        def _():
            kv[0, rs, :] = t

        for kk in range(4):
            @pl.when(k == kk)
            def _():
                for copy in y_copies(kk)[0]:
                    copy.start()
                for j in range(4):
                    start = pl.multiple_of(_piece_rows(x, c, rows, kk, j), half)
                    pltpu.make_async_copy(qs.at[pl.ds(kk * step_rows + j * half, half)], q_out.at[pl.ds(start, half)], q_sem.at[0]).start()
                place(0, kk)
                if kk >= 1:
                    forward(kk - 1)
                if kk >= 2:
                    opposite(kk - 2)
        return carry

    lax.fori_loop(0, 4, step, 0)
    forward(3)
    opposite(2)
    opposite(3)
    if gather_tab:
        store = pltpu.make_async_copy(tab, tab_out, w_sem.at[3])
        store.start()
        store.wait()
        _gather_end(t_ring, t_relay)
    pltpu.make_async_copy(qs, q_out, q_sem.at[0]).wait()
    for s, base in enumerate(bases):
        span = pl.ds(pl.multiple_of(base, shard), shard)
        pltpu.make_async_copy(kv.at[s], kv_out.at[c, span], l_sem.at[s]).wait()
        swap = _copy(kv.at[s], kv_out.at[c, span], (p_send, p_recv), s, "tp", sib)
        swap.wait_send()
        swap.wait_recv()
    for k in range(4):
        first, second = y_copies(k)
        for copy in first + second:
            copy.wait_send()
    _gather_end(ring, relay)


def _qkv(layer, windowed, shards, x, gain, tab, w_q, w_kv):
    rows, model = x.shape
    hd = w_q.shape[2]
    gather_tab = tab.ndim == 2
    shard = 8 * rows
    held = 2 if windowed else shards
    vmem, hbm = pl.BlockSpec(memory_space=pltpu.VMEM), pl.BlockSpec(memory_space=pl.ANY)
    tab_shape = (4, 2 * rows, hd)
    out_shape = [jax.ShapeDtypeStruct((shard, hd), BF16), jax.ShapeDtypeStruct((2, held * shard, hd), BF16)]
    if gather_tab:
        out_shape.append(jax.ShapeDtypeStruct(tab_shape, F32))
    return pl.pallas_call(
        functools.partial(_qkv_kernel, layer, gather_tab, windowed, shards),
        name=f"qkv_{layer}",
        out_shape=out_shape,
        in_specs=[vmem, vmem, hbm, hbm, hbm],
        out_specs=[hbm] * len(out_shape),
        scratch_shapes=[
            pltpu.VMEM((4, 2 * rows, model), BF16),
            pltpu.VMEM(tab_shape, F32),
            pltpu.VMEM((model, hd), BF16),
            pltpu.VMEM((model, hd), BF16),
            pltpu.VMEM((shard, hd), BF16),
            pltpu.VMEM((held, shard, hd), BF16),
            pltpu.SemaphoreType.DMA((10,)),
            pltpu.SemaphoreType.DMA((10,)),
            pltpu.SemaphoreType.DMA((10,)),
            pltpu.SemaphoreType.DMA((10,)),
            pltpu.SemaphoreType.DMA((16,)),
            pltpu.SemaphoreType.DMA((16,)),
            pltpu.SemaphoreType.DMA((4,)),
            pltpu.SemaphoreType.DMA((4,)),
            pltpu.SemaphoreType.DMA((4,)),
            pltpu.SemaphoreType.DMA((1,)),
            pltpu.SemaphoreType.DMA((4,)),
        ],
        compiler_params=_params(4 + layer),
    )(x, gain, tab, w_q, w_kv)


def _attend_kernel(scale, bounds, q_ref, lo_ref, kv_ref, o_ref, m_sc, l_sc, acc_sc):
    i = pl.program_id(0)
    rows, hd = q_ref.shape
    m_sc[...] = jnp.full(m_sc.shape, -1e30, F32)
    l_sc[...] = jnp.zeros(l_sc.shape, F32)
    acc_sc[...] = jnp.zeros(acc_sc.shape, F32)
    first = bounds[4, i]

    def block(masked, b, carry):
        start = pl.multiple_of(b * K_BLOCK, K_BLOCK)
        k = kv_ref[0, pl.ds(start, K_BLOCK), :]
        v = kv_ref[1, pl.ds(start, K_BLOCK), :]
        s = lax.dot_general(q_ref[...], k, (((1,), (1,)), ((), ())), preferred_element_type=F32)
        if masked:
            j = start + lax.broadcasted_iota(jnp.int32, (rows, K_BLOCK), 1)
            r = first + lax.broadcasted_iota(jnp.int32, (rows, K_BLOCK), 0)
            s = jnp.where((j <= r) & (j >= lo_ref[...]), s, -1e30)
        m_old = m_sc[...]
        m_new = jnp.maximum(m_old, jnp.max(s, axis=1, keepdims=True))
        p = jnp.exp2((s - m_new) * scale)
        alpha = jnp.exp2((m_old - m_new) * scale)
        m_sc[...] = m_new
        l_sc[...] = l_sc[...] * alpha + jnp.sum(p, axis=1, keepdims=True)
        acc_sc[...] = acc_sc[...] * alpha + jnp.dot(p.astype(BF16), v, preferred_element_type=F32)
        return carry

    lax.fori_loop(bounds[0, i], bounds[1, i], functools.partial(block, True), 0)
    lax.fori_loop(bounds[1, i], bounds[2, i], functools.partial(block, False), 0)
    lax.fori_loop(bounds[2, i], bounds[3, i], functools.partial(block, True), 0)
    o_ref[...] = (acc_sc[...] / l_sc[...]).astype(BF16)


def _attend(q, kv, row_lo, first_row):
    total, hd = q.shape
    blocks = total // Q_BLOCK
    lo2 = row_lo.reshape(blocks, Q_BLOCK)
    first = first_row + jnp.arange(blocks, dtype=jnp.int32) * Q_BLOCK
    b_lo = lo2[:, 0] // K_BLOCK
    b_hi = (first + Q_BLOCK - 1) // K_BLOCK + 1
    b_a = jnp.clip((lo2[:, -1] + K_BLOCK - 1) // K_BLOCK, b_lo, b_hi)
    b_b = jnp.clip((first + 1) // K_BLOCK, b_a, b_hi)
    bounds = jnp.stack([b_lo, b_a, b_b, b_hi, first]).astype(jnp.int32)
    return pl.pallas_call(
        functools.partial(_attend_kernel, hd ** -0.5 * math.log2(math.e)),
        name="attend",
        out_shape=jax.ShapeDtypeStruct((total, hd), BF16),
        grid_spec=pltpu.PrefetchScalarGridSpec(
            num_scalar_prefetch=1,
            grid=(blocks,),
            in_specs=[
                pl.BlockSpec((Q_BLOCK, hd), lambda i, b: (i, 0)),
                pl.BlockSpec((Q_BLOCK, 1), lambda i, b: (i, 0)),
                pl.BlockSpec(memory_space=pltpu.VMEM),
            ],
            out_specs=pl.BlockSpec((Q_BLOCK, hd), lambda i, b: (i, 0)),
            scratch_shapes=[pltpu.VMEM((Q_BLOCK, 1), F32), pltpu.VMEM((Q_BLOCK, 1), F32), pltpu.VMEM((Q_BLOCK, hd), F32)],
        ),
        compiler_params=pltpu.CompilerParams(dimension_semantics=("arbitrary",), vmem_limit_bytes=VMEM_LIMIT),
    )(bounds, q, row_lo.reshape(total, 1), kv)


def solution(mesh):
    tp_size, shards = mesh.shape["tp"], mesh.shape["sp"]
    row_spec = P(("dp", "sp", "tp"), None)
    id_spec = P(("dp", "sp", "tp"))
    whole = P()
    in_specs = (row_spec, id_spec, id_spec, whole, P(None, None, "tp", None), whole, whole, P(None, "tp", None, None), whole, P(None, None, "tp"), P(None, None, "tp"), P(None, "tp", None))

    def local_fn(x, segment_ids, positions, g_attn, w_q, w_k, w_v, w_o, g_mlp, w_gate, w_up, w_down):
        sp_idx = lax.axis_index("sp")
        tp_idx = lax.axis_index("tp")
        layers, model, heads_loc, hd = w_q.shape
        rows = x.shape[0]
        shard = rows * tp_size
        kv_head = tp_idx * w_k.shape[2] // tp_size
        inv_freq = ROPE_BASE ** (-jnp.arange(hd // 2, dtype=F32) / (hd // 2))
        angles = positions.astype(F32)[:, None] * inv_freq[None, :]
        tab = jnp.concatenate([jnp.cos(angles), jnp.sin(angles)], axis=1)
        seg_all = lax.all_gather(segment_ids, ("sp", "tp"), tiled=True)
        second, third = jnp.sum(seg_all < 1), jnp.sum(seg_all < 2)
        token = sp_idx * shard + jnp.arange(shard, dtype=jnp.int32)
        seg_lo = jnp.where(token >= third, third, jnp.where(token >= second, second, 0)).astype(jnp.int32)
        pick_k = lax.dynamic_slice_in_dim(w_k, kv_head, 1, 2).reshape(layers, model, hd)
        pick_v = lax.dynamic_slice_in_dim(w_v, kv_head, 1, 2).reshape(layers, model, hd)
        w_kv = jnp.where(tp_idx % 2 == 0, pick_k, pick_v)
        w_q2 = w_q.reshape(layers, model, hd)
        w_o2 = w_o.reshape(layers, hd, model)
        for layer in range(layers):
            windowed = layer % 2 == 0
            got = _qkv(layer, windowed, shards, x, g_attn[layer:layer + 1], tab, w_q2, w_kv)
            q, kv = got[0], got[1]
            if len(got) == 3:
                tab = got[2]
            if windowed:
                shift = (sp_idx - 1) * shard
                row_lo = jnp.maximum(seg_lo, token - (WINDOW - 1)) - shift
            else:
                shift = 0
                row_lo = seg_lo
            mixed = _attend(q, kv, row_lo, sp_idx * shard - shift)
            hidden = _out_proj(layer, mixed, x, w_o2)
            x = _mlp(layer, hidden, g_mlp[layer:layer + 1], w_gate, w_up, w_down)
        return x

    return jax.shard_map(local_fn, mesh=mesh, in_specs=in_specs, out_specs=row_spec, check_vma=False)
```

```python
import functools
import math

import jax
import jax.numpy as jnp
from jax import lax
from jax.experimental import pallas as pl
from jax.experimental.pallas import tpu as pltpu
from jax.sharding import PartitionSpec as P

EPS = 1e-6
ROPE_BASE = 10000.0
WINDOW = 1024
CHIPS = 4
MESH = pl.DeviceIdType.MESH
BF16 = jnp.bfloat16
F32 = jnp.float32
VMEM_LIMIT = 66_000_000
UP_TILE = 1280
DOWN_TILE = 2560


def _place():
    t = lax.axis_index("tp")
    c = lax.rem(t, 2)
    x = t // 2
    right = lax.rem(x + 1, CHIPS) * 2 + c
    left = lax.rem(x + CHIPS - 1, CHIPS) * 2 + c
    sib = x * 2 + 1 - c
    return x, c, right, left, sib


def _copy(src, dst, sems, index, axis, dev):
    send, recv = sems
    return pltpu.make_async_remote_copy(
        src_ref=src, dst_ref=dst, send_sem=send.at[index], recv_sem=recv.at[index],
        device_id={axis: dev}, device_id_type=MESH)


def _barrier(peers):
    bar = pltpu.get_barrier_semaphore()
    for axis, dev in peers:
        pl.semaphore_signal(bar, inc=1, device_id={axis: dev}, device_id_type=MESH)
    pl.semaphore_wait(bar, len(peers))


def _piece_rows(x, c, rows, k, j):
    half = rows // 2
    core = c if j < 2 else 1 - c
    even = j % 2 == 0
    if k == 0:
        chip, h = x, j % 2
    elif k == 1:
        chip, h = (x + CHIPS - 1, 0) if even else (x + 1, 1)
    elif k == 2:
        chip, h = x + 2, j % 2
    else:
        chip, h = (x + CHIPS - 1, 1) if even else (x + 1, 0)
    return lax.rem(chip, CHIPS) * (2 * rows) + core * rows + h * half


def _gather_copies(buf, sems, rows, right, left, sib):
    half, part = rows // 2, rows // 4
    a, b = pl.ds(0, half), pl.ds(half, half)
    a1, a2, b1, b2 = (pl.ds(i * part, part) for i in range(4))
    ring = [
        _copy(buf.at[0, a], buf.at[1, a], sems, 0, "tp", right),
        _copy(buf.at[0, b], buf.at[1, b], sems, 1, "tp", left),
        _copy(buf.at[0, b1], buf.at[3, a1], sems, 2, "tp", right),
        _copy(buf.at[0, a1], buf.at[3, b1], sems, 3, "tp", left),
        _copy(buf.at[1, a], buf.at[2, a], sems, 4, "tp", right),
        _copy(buf.at[1, b], buf.at[2, b], sems, 5, "tp", left),
        _copy(buf.at[0, b2], buf.at[3, a2], sems, 6, "tp", right),
        _copy(buf.at[0, a2], buf.at[3, b2], sems, 7, "tp", left),
    ]
    relay = [_copy(buf.at[k, pl.ds(0, rows)], buf.at[k, pl.ds(rows, rows)], sems, 8 + k, "tp", sib) for k in range(4)]
    return ring, relay


def _gather_begin(*gathers):
    for i in (0, 1):
        for ring, relay in gathers:
            ring[i].start()
    for ring, relay in gathers:
        relay[0].start()
    for i in (2, 3):
        for ring, relay in gathers:
            ring[i].start()


def _gather_arrive(k, *gathers):
    if k == 1:
        for i in (0, 1):
            for ring, relay in gathers:
                ring[i].wait_recv()
                ring[4 + i].start()
        for i in (6, 7):
            for ring, relay in gathers:
                ring[i].start()
    for ring, relay in gathers:
        for i in {2: (4, 5), 3: (2, 3, 6, 7)}.get(k, ()):
            ring[i].wait_recv()
        if k >= 1:
            relay[k].start()
    for ring, relay in gathers:
        relay[k].wait_recv()


def _gather_end(ring, relay):
    for copy in ring + relay:
        copy.wait_send()


def _norm_into(dst, x_ref, g_ref):
    rows = x_ref.shape[0]
    gain = g_ref[...].astype(F32)
    chunk = 16

    def body(i, carry):
        rs = pl.ds(pl.multiple_of(i * chunk, chunk), chunk)
        wide = x_ref[rs, :].astype(F32)
        inv = lax.rsqrt(jnp.mean(wide * wide, axis=-1, keepdims=True) + EPS)
        dst[0, rs, :] = (wide * inv * gain).astype(BF16)
        return carry

    lax.fori_loop(0, rows // chunk, body, 0)


def _add_rows(rows, body):
    chunk = 16

    def step(i, carry):
        body(pl.ds(pl.multiple_of(i * chunk, chunk), chunk))
        return carry

    lax.fori_loop(0, rows // chunk, step, 0)


class _Scatter:
    def __init__(self, part, from_sib, direct, chain, last, sems, rows, right, left, sib):
        half = rows // 2
        a, b = pl.ds(0, half), pl.ds(half, half)
        self.rows, self.part, self.from_sib = rows, part, from_sib
        self.direct, self.chain, self.last = direct, chain, last
        self.swap = [_copy(part.at[k, pl.ds(rows, rows)], from_sib.at[k], sems, k, "tp", sib) for k in range(4)]
        self.d = [_copy(part.at[1, b], direct.at[b], sems, 4, "tp", right), _copy(part.at[1, a], direct.at[a], sems, 5, "tp", left)]
        self.c = [_copy(part.at[2, a], chain.at[b], sems, 6, "tp", right), _copy(part.at[2, b], chain.at[a], sems, 7, "tp", left)]
        self.l = [_copy(part.at[3, b], last.at[a], sems, 8, "tp", right), _copy(part.at[3, a], last.at[b], sems, 9, "tp", left)]

    def _fold(self, k, extra=None):
        part, from_sib = self.part, self.from_sib

        def body(rs):
            total = part[k, rs, :].astype(F32) + from_sib[k, rs, :].astype(F32)
            if extra is not None:
                total = total + extra[rs, :].astype(F32)
            part[k, rs, :] = total.astype(BF16)

        _add_rows(self.rows, body)

    def send_direct(self):
        self.swap[1].wait_recv()
        self._fold(1)
        for copy in self.d:
            copy.start()

    def send_chain(self):
        self.swap[2].wait_recv()
        self._fold(2)
        for copy in self.c:
            copy.start()

    def forward_chain(self):
        self.swap[3].wait_recv()
        for copy in self.c:
            copy.wait_recv()
        self._fold(3, self.chain)
        for copy in self.l:
            copy.start()

    def finish(self, o_ref, x_ref):
        self.swap[0].wait_recv()
        for copy in self.d + self.l:
            copy.wait_recv()
        part, from_sib, direct, last = self.part, self.from_sib, self.direct, self.last

        def body(rs):
            total = part[0, rs, :].astype(F32) + from_sib[0, rs, :].astype(F32)
            total = total + direct[rs, :].astype(F32) + last[rs, :].astype(F32)
            o_ref[rs, :] = (x_ref[rs, :].astype(F32) + total.astype(BF16).astype(F32)).astype(BF16)

        _add_rows(self.rows, body)
        for copy in self.swap + self.d + self.c + self.l:
            copy.wait_send()


def _scatter_scratch(rows, model):
    return [
        pltpu.VMEM((4, 2 * rows, model), BF16),
        pltpu.VMEM((4, rows, model), BF16),
        pltpu.VMEM((rows, model), BF16),
        pltpu.VMEM((rows, model), BF16),
        pltpu.VMEM((rows, model), BF16),
        pltpu.SemaphoreType.DMA((10,)),
        pltpu.SemaphoreType.DMA((10,)),
    ]


def _params(collective_id):
    return pltpu.CompilerParams(collective_id=collective_id, has_side_effects=True, vmem_limit_bytes=VMEM_LIMIT)


def _mlp_kernel(layer, x_ref, g_ref, wg_hbm, wu_hbm, wd_hbm, o_ref, buf, wgu, wd, act, part, from_sib, direct, chain, last,
                s_send, s_recv, g_send, g_recv, w_sem):
    rows, model = x_ref.shape
    cols = act.shape[1]
    tiles = cols // UP_TILE
    x, c, right, left, sib = _place()

    def load(i, n):
        src = (wg_hbm, wu_hbm)[i].at[layer, :, pl.ds(n * UP_TILE, UP_TILE)]
        return pltpu.make_async_copy(src, wgu.at[:, pl.ds((2 * n + i) * UP_TILE, UP_TILE)], w_sem.at[2 * n + i])

    load_down = pltpu.make_async_copy(wd_hbm.at[layer], wd, w_sem.at[2 * tiles])
    for n in range(tiles):
        load(0, n).start()
        load(1, n).start()
    load_down.start()
    _norm_into(buf, x_ref, g_ref)
    _barrier((("tp", left), ("tp", right), ("tp", sib)))
    gather = _gather_copies(buf, (g_send, g_recv), rows, right, left, sib)
    _gather_begin(gather)
    scatter = _Scatter(part, from_sib, direct, chain, last, (s_send, s_recv), rows, right, left, sib)
    for n in range(tiles):
        load(0, n).wait()
        load(1, n).wait()

    def step(k, carry):
        for kk in range(4):
            @pl.when(k == kk)
            def _():
                _gather_arrive(kk, gather)

        def up(n, inner):
            cs = pl.ds(pl.multiple_of(n * 2 * UP_TILE, 2 * UP_TILE), 2 * UP_TILE)
            both = jnp.dot(buf[k], wgu[:, cs], preferred_element_type=F32)
            gate, lin = both[:, :UP_TILE], both[:, UP_TILE:]
            act[:, pl.ds(pl.multiple_of(n * UP_TILE, UP_TILE), UP_TILE)] = (jax.nn.silu(gate) * lin).astype(BF16)
            return inner

        lax.fori_loop(0, tiles, up, 0)

        @pl.when(k == 0)
        def _():
            load_down.wait()

        def down(n, inner):
            cs = pl.ds(pl.multiple_of(n * DOWN_TILE, DOWN_TILE), DOWN_TILE)
            part[k, :, cs] = jnp.dot(act[...], wd[:, cs], preferred_element_type=F32).astype(BF16)
            return inner

        lax.fori_loop(0, model // DOWN_TILE, down, 0)
        for kk in range(4):
            @pl.when(k == kk)
            def _():
                scatter.swap[kk].start()
                if kk == 1:
                    scatter.send_direct()
                if kk == 2:
                    scatter.send_chain()
        return carry

    lax.fori_loop(0, 4, step, 0)
    scatter.forward_chain()
    scatter.finish(o_ref, x_ref)
    _gather_end(*gather)


def _mlp(layer, x, gain, w_gate, w_up, w_down):
    rows, model = x.shape
    cols = w_gate.shape[2]
    vmem, hbm = pl.BlockSpec(memory_space=pltpu.VMEM), pl.BlockSpec(memory_space=pl.ANY)
    return pl.pallas_call(
        functools.partial(_mlp_kernel, layer),
        name=f"mlp_{layer}",
        out_shape=jax.ShapeDtypeStruct((rows, model), BF16),
        in_specs=[vmem, vmem, hbm, hbm, hbm],
        out_specs=vmem,
        scratch_shapes=[
            pltpu.VMEM((4, 2 * rows, model), BF16),
            pltpu.VMEM((model, 2 * cols), BF16),
            pltpu.VMEM((cols, model), BF16),
            pltpu.VMEM((2 * rows, cols), BF16),
            *_scatter_scratch(rows, model),
            pltpu.SemaphoreType.DMA((12,)),
            pltpu.SemaphoreType.DMA((12,)),
            pltpu.SemaphoreType.DMA((2 * (cols // UP_TILE) + 1,)),
        ],
        compiler_params=_params(layer),
    )(x, gain, w_gate, w_up, w_down)


def _out_kernel(layer, m_ref, x_ref, wo_hbm, o_ref, wo, lhs, part, from_sib, direct, chain, last, s_send, s_recv, w_sem):
    rows, model = x_ref.shape
    half = rows // 2
    x, c, right, left, sib = _place()
    load = pltpu.make_async_copy(wo_hbm.at[layer], wo, w_sem.at[0])
    load.start()
    _barrier((("tp", left), ("tp", right), ("tp", sib)))
    scatter = _Scatter(part, from_sib, direct, chain, last, (s_send, s_recv), rows, right, left, sib)
    load.wait()
    nt = 512
    for k in (2, 1, 3, 0):
        for j in range(4):
            start = pl.multiple_of(_piece_rows(x, c, rows, k, j), half)
            lhs[pl.ds(j * half, half), :] = m_ref[pl.ds(start, half), :]

        def down(n, inner):
            cs = pl.ds(pl.multiple_of(n * nt, nt), nt)
            part[k, :, cs] = jnp.dot(lhs[...], wo[:, cs], preferred_element_type=F32).astype(BF16)
            return inner

        lax.fori_loop(0, model // nt, down, 0)
        scatter.swap[k].start()
        if k == 2:
            scatter.send_chain()
        if k == 1:
            scatter.send_direct()
    scatter.forward_chain()
    scatter.finish(o_ref, x_ref)


def _out_proj(layer, mixed, x, w_o):
    rows, model = x.shape
    head_dim = mixed.shape[1]
    vmem, hbm = pl.BlockSpec(memory_space=pltpu.VMEM), pl.BlockSpec(memory_space=pl.ANY)
    return pl.pallas_call(
        functools.partial(_out_kernel, layer),
        name=f"out_{layer}",
        out_shape=jax.ShapeDtypeStruct((rows, model), BF16),
        in_specs=[vmem, vmem, hbm],
        out_specs=vmem,
        scratch_shapes=[
            pltpu.VMEM((head_dim, model), BF16),
            pltpu.VMEM((2 * rows, head_dim), BF16),
            *_scatter_scratch(rows, model),
            pltpu.SemaphoreType.DMA((1,)),
        ],
        compiler_params=_params(2 + layer),
    )(mixed, x, w_o)


def _qkv_kernel(layer, gather_tab, windowed, shards, x_ref, g_ref, tab_in, wq_hbm, wkv_hbm, *rest):
    if gather_tab:
        n_ref, q_out, kv_out, tab_out, n_out = rest[:5]
        n_y, n_x, n_send, n_recv, c_send, c_recv = rest[5:11]
        rest = rest[11:]
    else:
        q_out, kv_out = rest[:2]
        rest = rest[2:]
    buf, tab, wq, wkv, qs, kv, g_send, g_recv, t_send, t_recv, y_send, y_recv, p_send, p_recv, l_sem, q_sem, w_sem = rest
    rows, model = x_ref.shape
    half, step_rows = rows // 2, 2 * rows
    shard = 4 * step_rows
    hd = wq.shape[1]
    x, c, right, left, sib = _place()
    y = lax.axis_index("sp")
    up, down = lax.rem(y + 1, shards), lax.rem(y + shards - 1, shards)
    loads = [pltpu.make_async_copy(wq_hbm.at[layer], wq, w_sem.at[0]), pltpu.make_async_copy(wkv_hbm.at[layer], wkv, w_sem.at[1])]
    for load in loads:
        load.start()
    if not gather_tab:
        tab_load = pltpu.make_async_copy(tab_in, tab, w_sem.at[2])
        tab_load.start()
    else:
        tab_load = pltpu.make_async_copy(tab_in, tab.at[0, pl.ds(0, rows)], w_sem.at[2])
        tab_load.start()
    _norm_into(buf, x_ref, g_ref)
    if gather_tab:
        n_y[0] = n_ref[...]
    tab_load.wait()
    _barrier((("tp", left), ("tp", right), ("tp", sib), ("sp", up), ("sp", down)))
    gather = _gather_copies(buf, (g_send, g_recv), rows, right, left, sib)
    gathers = [gather]
    if gather_tab:
        gathers.insert(0, _gather_copies(tab, (t_send, t_recv), rows, right, left, sib))
        n_copies = [_copy(n_y.at[src], n_y.at[dst], (c_send, c_recv), i, "sp", dev) for i, (src, dst, dev) in enumerate(((0, 1, up), (0, 2, down), (1, 3, up)))]
        n_copies[0].start()
        n_copies[1].start()
    _gather_begin(*gathers)
    if gather_tab:
        n_copies[0].wait_recv()
        n_copies[2].start()
        n_copies[1].wait_recv()
        n_copies[2].wait_recv()
        n_x[0, :32, :] = jnp.zeros((32, 128), F32)
        n_x[0, :8, :] = n_y[0] + n_y[1] + n_y[2] + n_y[3]
        gathers.append(_gather_copies(n_x, (n_send, n_recv), 32, right, left, sib))
        _gather_begin(gathers[2])

    if windowed:
        bases = (shard, 0)
    else:
        bases = tuple(lax.rem(y + d, shards) * shard for d in (0, shards - 1, 1, 2))

    def y_copies(k):
        whole, a, b = pl.ds(k * step_rows, step_rows), pl.ds(k * step_rows, rows), pl.ds(k * step_rows + rows, rows)
        sems = (y_send, y_recv)
        first = [_copy(kv.at[0, whole], kv.at[1, whole], sems, 4 * k, "sp", up)]
        second = []
        if not windowed:
            first.append(_copy(kv.at[0, whole], kv.at[2, whole], sems, 4 * k + 1, "sp", down))
            second.append(_copy(kv.at[1, a], kv.at[3, a], sems, 4 * k + 2, "sp", up))
            second.append(_copy(kv.at[2, b], kv.at[3, b], sems, 4 * k + 3, "sp", down))
        return first, second

    def place(s, k):
        for j in range(4):
            src = kv.at[s, pl.ds(k * step_rows + j * half, half)]
            start = pl.multiple_of(bases[s] + _piece_rows(x, c, rows, k, j), half)
            dst = kv_out.at[c, pl.ds(start, half)]
            pltpu.make_async_copy(src, dst, l_sem.at[s]).start()
            _copy(src, dst, (p_send, p_recv), s, "tp", sib).start()

    def forward(k):
        first, second = y_copies(k)
        for copy in first:
            copy.wait_recv()
        for copy in second:
            copy.start()
        place(1, k)
        if not windowed:
            place(2, k)

    def opposite(k):
        first, second = y_copies(k)
        for copy in second:
            copy.wait_recv()
        if second:
            place(3, k)

    def step(k, carry):
        for kk in range(4):
            @pl.when(k == kk)
            def _():
                if kk == 0:
                    loads[0].wait()
                    loads[1].wait()
                _gather_arrive(kk, *gathers)

        cos, sin = tab[k, :, :hd // 2], tab[k, :, hd // 2:]

        def rotate(t):
            lower, upper = t[:, :hd // 2], t[:, hd // 2:]
            return jnp.concatenate([lower * cos - upper * sin, upper * cos + lower * sin], axis=-1).astype(BF16)

        q = jnp.dot(buf[k], wq[...], preferred_element_type=F32).astype(BF16).astype(F32)
        rs = pl.ds(pl.multiple_of(k * step_rows, step_rows), step_rows)
        qs[rs, :] = rotate(q)
        t = jnp.dot(buf[k], wkv[...], preferred_element_type=F32).astype(BF16)

        @pl.when(c == 0)
        def _():
            kv[0, rs, :] = rotate(t.astype(F32))

        @pl.when(c == 1)
        def _():
            kv[0, rs, :] = t

        for kk in range(4):
            @pl.when(k == kk)
            def _():
                for copy in y_copies(kk)[0]:
                    copy.start()
                for j in range(4):
                    start = pl.multiple_of(_piece_rows(x, c, rows, kk, j), half)
                    pltpu.make_async_copy(qs.at[pl.ds(kk * step_rows + j * half, half)], q_out.at[pl.ds(start, half)], q_sem.at[0]).start()
                place(0, kk)
                if kk >= 1:
                    forward(kk - 1)
                if kk >= 2:
                    opposite(kk - 2)
        return carry

    lax.fori_loop(0, 4, step, 0)
    forward(3)
    opposite(2)
    opposite(3)
    if gather_tab:
        store = pltpu.make_async_copy(tab, tab_out, w_sem.at[3])
        store.start()
        store.wait()
        total = n_x[0, :8, :]
        for k in range(4):
            for i in range(8):
                if k or i:
                    total = total + n_x[k, 8 * i:8 * i + 8, :]
        n_out[...] = total
        for copy in n_copies:
            copy.wait_send()
    pltpu.make_async_copy(qs, q_out, q_sem.at[0]).wait()
    for s, base in enumerate(bases):
        span = pl.ds(pl.multiple_of(base, shard), shard)
        pltpu.make_async_copy(kv.at[s], kv_out.at[c, span], l_sem.at[s]).wait()
        swap = _copy(kv.at[s], kv_out.at[c, span], (p_send, p_recv), s, "tp", sib)
        swap.wait_send()
        swap.wait_recv()
    for k in range(4):
        first, second = y_copies(k)
        for copy in first + second:
            copy.wait_send()
    for ring, relay in gathers:
        _gather_end(ring, relay)


def _qkv(layer, windowed, shards, x, gain, tab, w_q, w_kv, counts):
    rows, model = x.shape
    hd = w_q.shape[2]
    gather_tab = tab.ndim == 2
    shard = 8 * rows
    held = 2 if windowed else shards
    vmem, hbm = pl.BlockSpec(memory_space=pltpu.VMEM), pl.BlockSpec(memory_space=pl.ANY)
    tab_shape = (4, 2 * rows, hd)
    out_shape = [jax.ShapeDtypeStruct((shard, hd), BF16), jax.ShapeDtypeStruct((2, held * shard, hd), BF16)]
    if gather_tab:
        out_shape += [jax.ShapeDtypeStruct(tab_shape, F32), jax.ShapeDtypeStruct(counts.shape, F32)]
    dma = pltpu.SemaphoreType.DMA
    count_scratch = [pltpu.VMEM((4, *counts.shape), F32), pltpu.VMEM((4, 64, 128), F32), dma((12,)), dma((12,)), dma((3,)), dma((3,))]
    return pl.pallas_call(
        functools.partial(_qkv_kernel, layer, gather_tab, windowed, shards),
        name=f"qkv_{layer}",
        out_shape=out_shape,
        in_specs=[vmem, vmem, hbm, hbm, hbm] + [vmem] * gather_tab,
        out_specs=[hbm] * 3 + [vmem] if gather_tab else [hbm] * 2,
        scratch_shapes=[
            *(count_scratch if gather_tab else []),
            pltpu.VMEM((4, 2 * rows, model), BF16),
            pltpu.VMEM(tab_shape, F32),
            pltpu.VMEM((model, hd), BF16),
            pltpu.VMEM((model, hd), BF16),
            pltpu.VMEM((shard, hd), BF16),
            pltpu.VMEM((held, shard, hd), BF16),
            pltpu.SemaphoreType.DMA((12,)),
            pltpu.SemaphoreType.DMA((12,)),
            pltpu.SemaphoreType.DMA((12,)),
            pltpu.SemaphoreType.DMA((12,)),
            pltpu.SemaphoreType.DMA((16,)),
            pltpu.SemaphoreType.DMA((16,)),
            pltpu.SemaphoreType.DMA((4,)),
            pltpu.SemaphoreType.DMA((4,)),
            pltpu.SemaphoreType.DMA((4,)),
            pltpu.SemaphoreType.DMA((1,)),
            pltpu.SemaphoreType.DMA((4,)),
        ],
        compiler_params=_params(4 + layer),
    )(x, gain, tab, w_q, w_kv, *([counts] if gather_tab else []))


def _attend_kernel(scale, k_block, bounds, q_ref, lo_ref, kv_ref, o_ref, m_sc, l_sc, acc_sc):
    i = pl.program_id(0)
    rows, hd = q_ref.shape
    m_sc[...] = jnp.full(m_sc.shape, -1e30, F32)
    l_sc[...] = jnp.zeros(l_sc.shape, F32)
    acc_sc[...] = jnp.zeros(acc_sc.shape, F32)
    first = bounds[4, i]

    def block(masked, b, carry):
        start = pl.multiple_of(b * k_block, k_block)
        k = kv_ref[0, pl.ds(start, k_block), :]
        v = kv_ref[1, pl.ds(start, k_block), :]
        s = lax.dot_general(k, q_ref[...], (((1,), (1,)), ((), ())), preferred_element_type=F32)
        if masked:
            j = start + lax.broadcasted_iota(jnp.int32, (k_block, rows), 0)
            r = first + lax.broadcasted_iota(jnp.int32, (k_block, rows), 1)
            s = jnp.where((j <= r) & (j >= lo_ref[...]), s, -1e30)
        m_old = m_sc[...]
        m_new = jnp.maximum(m_old, jnp.max(s, axis=0, keepdims=True))
        p = jnp.exp2((s - m_new) * scale)
        alpha = jnp.exp2((m_old - m_new) * scale)
        m_sc[...] = m_new
        l_sc[...] = l_sc[...] * alpha + jnp.sum(p, axis=0, keepdims=True)
        add = lax.dot_general(v, p.astype(BF16), (((0,), (0,)), ((), ())), preferred_element_type=F32)
        acc_sc[...] = acc_sc[...] * alpha + add
        return carry

    lax.fori_loop(bounds[0, i], bounds[1, i], functools.partial(block, True), 0)
    lax.fori_loop(bounds[1, i], bounds[2, i], functools.partial(block, False), 0)
    lax.fori_loop(bounds[2, i], bounds[3, i], functools.partial(block, True), 0)
    o_ref[...] = jnp.transpose(acc_sc[...] / l_sc[...]).astype(BF16)


def _attend(q, kv, row_lo, first_row, block):
    total, hd = q.shape
    blocks = total // block
    lo2 = row_lo.reshape(blocks, block)
    first = first_row + jnp.arange(blocks, dtype=jnp.int32) * block
    b_lo = lo2[:, 0] // block
    b_hi = (first + block - 1) // block + 1
    b_a = jnp.clip((lo2[:, -1] + block - 1) // block, b_lo, b_hi)
    b_b = jnp.clip((first + 1) // block, b_a, b_hi)
    bounds = jnp.stack([b_lo, b_a, b_b, b_hi, first]).astype(jnp.int32)
    return pl.pallas_call(
        functools.partial(_attend_kernel, hd ** -0.5 * math.log2(math.e), block),
        name="attend",
        out_shape=jax.ShapeDtypeStruct((total, hd), BF16),
        grid_spec=pltpu.PrefetchScalarGridSpec(
            num_scalar_prefetch=1,
            grid=(blocks,),
            in_specs=[
                pl.BlockSpec((block, hd), lambda i, b: (i, 0)),
                pl.BlockSpec((1, block), lambda i, b: (0, i)),
                pl.BlockSpec(memory_space=pltpu.VMEM),
            ],
            out_specs=pl.BlockSpec((block, hd), lambda i, b: (i, 0)),
            scratch_shapes=[pltpu.VMEM((1, block), F32), pltpu.VMEM((1, block), F32), pltpu.VMEM((hd, block), F32)],
        ),
        compiler_params=pltpu.CompilerParams(dimension_semantics=("arbitrary",), vmem_limit_bytes=VMEM_LIMIT),
    )(bounds, q, row_lo.reshape(1, total), kv)


def solution(mesh):
    tp_size, shards = mesh.shape["tp"], mesh.shape["sp"]
    row_spec = P(("dp", "sp", "tp"), None)
    id_spec = P(("dp", "sp", "tp"))
    whole = P()
    in_specs = (row_spec, id_spec, id_spec, whole, P(None, None, "tp", None), whole, whole, P(None, "tp", None, None), whole, P(None, None, "tp"), P(None, None, "tp"), P(None, "tp", None))

    def local_fn(x, segment_ids, positions, g_attn, w_q, w_k, w_v, w_o, g_mlp, w_gate, w_up, w_down):
        sp_idx = lax.axis_index("sp")
        tp_idx = lax.axis_index("tp")
        layers, model, heads_loc, hd = w_q.shape
        rows = x.shape[0]
        shard = rows * tp_size
        kv_head = tp_idx * w_k.shape[2] // tp_size
        inv_freq = ROPE_BASE ** (-jnp.arange(hd // 2, dtype=F32) / (hd // 2))
        angles = positions.astype(F32)[:, None] * inv_freq[None, :]
        tab = jnp.concatenate([jnp.cos(angles), jnp.sin(angles)], axis=1)
        lane = lax.broadcasted_iota(jnp.int32, (8, 128), 1)
        counts = jnp.where(lane == 0, jnp.sum(segment_ids < 1), jnp.where(lane == 1, jnp.sum(segment_ids < 2), 0)).astype(F32)
        token = sp_idx * shard + jnp.arange(shard, dtype=jnp.int32)

        def pick(w):
            return lax.optimization_barrier(lax.dynamic_slice_in_dim(w, kv_head, 1, 2).reshape(layers, model, hd))

        w_kv = lax.cond(tp_idx % 2 == 0, lambda: pick(w_k), lambda: pick(w_v))
        w_q2 = w_q.reshape(layers, model, hd)
        w_o2 = w_o.reshape(layers, hd, model)
        for layer in range(layers):
            windowed = layer % 2 == 0
            got = _qkv(layer, windowed, shards, x, g_attn[layer:layer + 1], tab, w_q2, w_kv, counts)
            q, kv = got[0], got[1]
            if layer == 0:
                tab = got[2]
                second, third = got[3][0, 0].astype(jnp.int32), got[3][0, 1].astype(jnp.int32)
                seg_lo = jnp.where(token >= third, third, jnp.where(token >= second, second, 0))
            if windowed:
                shift = (sp_idx - 1) * shard
                row_lo = jnp.maximum(seg_lo, token - (WINDOW - 1)) - shift
            else:
                shift = 0
                row_lo = seg_lo
            mixed = _attend(q, kv, row_lo, sp_idx * shard - shift, 512 if windowed else 1024)
            hidden = _out_proj(layer, mixed, x, w_o2)
            x = _mlp(layer, hidden, g_mlp[layer:layer + 1], w_gate, w_up, w_down)
        return x

    return jax.shard_map(local_fn, mesh=mesh, in_specs=in_specs, out_specs=row_spec, check_vma=False)
```

```python
import functools
import math

import jax
import jax.numpy as jnp
from jax import lax
from jax.experimental import pallas as pl
from jax.experimental.pallas import tpu as pltpu
from jax.sharding import PartitionSpec as P

EPS = 1e-6
ROPE_BASE = 10000.0
WINDOW = 1024
CHIPS = 4
MESH = pl.DeviceIdType.MESH
BF16 = jnp.bfloat16
F32 = jnp.float32
VMEM_LIMIT = 66_000_000
UP_TILE = 1280
DOWN_TILE = 1280
OUT_TILE = 1280


def _place():
    t = lax.axis_index("tp")
    c = lax.rem(t, 2)
    x = t // 2
    right = lax.rem(x + 1, CHIPS) * 2 + c
    left = lax.rem(x + CHIPS - 1, CHIPS) * 2 + c
    sib = x * 2 + 1 - c
    return x, c, right, left, sib


def _copy(src, dst, sems, index, axis, dev):
    send, recv = sems
    return pltpu.make_async_remote_copy(
        src_ref=src, dst_ref=dst, send_sem=send.at[index], recv_sem=recv.at[index],
        device_id={axis: dev}, device_id_type=MESH)


def _greet(peers):
    bar = pltpu.get_barrier_semaphore()
    for axis, dev in peers:
        pl.semaphore_signal(bar, inc=1, device_id={axis: dev}, device_id_type=MESH)


def _meet(peers):
    pl.semaphore_wait(pltpu.get_barrier_semaphore(), len(peers))


def _piece_rows(x, c, rows, k, j):
    half = rows // 2
    core = c if j < 2 else 1 - c
    even = j % 2 == 0
    if k == 0:
        chip, h = x, j % 2
    elif k == 1:
        chip, h = (x + CHIPS - 1, 0) if even else (x + 1, 1)
    elif k == 2:
        chip, h = x + 2, j % 2
    else:
        chip, h = (x + CHIPS - 1, 1) if even else (x + 1, 0)
    return lax.rem(chip, CHIPS) * (2 * rows) + core * rows + h * half


def _gather_copies(buf, sems, rows, right, left, sib):
    half, part = rows // 2, rows // 4
    a, b = pl.ds(0, half), pl.ds(half, half)
    a1, a2, b1, b2 = (pl.ds(i * part, part) for i in range(4))
    ring = [
        _copy(buf.at[0, a], buf.at[1, a], sems, 0, "tp", right),
        _copy(buf.at[0, b], buf.at[1, b], sems, 1, "tp", left),
        _copy(buf.at[0, b1], buf.at[3, a1], sems, 2, "tp", right),
        _copy(buf.at[0, a1], buf.at[3, b1], sems, 3, "tp", left),
        _copy(buf.at[1, a], buf.at[2, a], sems, 4, "tp", right),
        _copy(buf.at[1, b], buf.at[2, b], sems, 5, "tp", left),
        _copy(buf.at[0, b2], buf.at[3, a2], sems, 6, "tp", right),
        _copy(buf.at[0, a2], buf.at[3, b2], sems, 7, "tp", left),
    ]
    relay = [_copy(buf.at[k, pl.ds(0, rows)], buf.at[k, pl.ds(rows, rows)], sems, 8 + k, "tp", sib) for k in range(4)]
    return ring, relay


def _gather_begin(*gathers):
    for i in (0, 1):
        for ring, relay in gathers:
            ring[i].start()
    for ring, relay in gathers:
        relay[0].start()
    for i in (2, 3):
        for ring, relay in gathers:
            ring[i].start()


def _gather_arrive(k, *gathers):
    if k == 1:
        for i in (0, 1):
            for ring, relay in gathers:
                ring[i].wait_recv()
                ring[4 + i].start()
        for i in (6, 7):
            for ring, relay in gathers:
                ring[i].start()
    for ring, relay in gathers:
        for i in {2: (4, 5), 3: (2, 3, 6, 7)}.get(k, ()):
            ring[i].wait_recv()
        if k >= 1:
            relay[k].start()


def _relay_arrive(k, *gathers):
    for ring, relay in gathers:
        relay[k].wait_recv()


def _gather_end(ring, relay):
    for copy in ring + relay:
        copy.wait_send()


def _norm_into(dst, x_ref, g_ref):
    rows = x_ref.shape[0]
    gain = g_ref[...].astype(F32)
    chunk = 16

    def body(i, carry):
        rs = pl.ds(pl.multiple_of(i * chunk, chunk), chunk)
        wide = x_ref[rs, :].astype(F32)
        inv = lax.rsqrt(jnp.mean(wide * wide, axis=-1, keepdims=True) + EPS)
        dst[0, rs, :] = (wide * inv * gain).astype(BF16)
        return carry

    lax.fori_loop(0, rows // chunk, body, 0)


def _add_rows(rows, body):
    chunk = 16

    def step(i, carry):
        body(pl.ds(pl.multiple_of(i * chunk, chunk), chunk))
        return carry

    lax.fori_loop(0, rows // chunk, step, 0)


class _Scatter:
    def __init__(self, part, from_sib, direct, chain, last, sems, rows, right, left, sib):
        half = rows // 2
        a, b = pl.ds(0, half), pl.ds(half, half)
        self.rows, self.part, self.from_sib = rows, part, from_sib
        self.direct, self.chain, self.last = direct, chain, last
        self.swap = [_copy(part.at[k, pl.ds(rows, rows)], from_sib.at[k], sems, k, "tp", sib) for k in range(4)]
        self.d = [_copy(part.at[1, b], direct.at[b], sems, 4, "tp", right), _copy(part.at[1, a], direct.at[a], sems, 5, "tp", left)]
        self.c = [_copy(part.at[2, a], chain.at[b], sems, 6, "tp", right), _copy(part.at[2, b], chain.at[a], sems, 7, "tp", left)]
        self.l = [_copy(part.at[3, b], last.at[a], sems, 8, "tp", right), _copy(part.at[3, a], last.at[b], sems, 9, "tp", left)]

    def _fold(self, k, extra=None):
        part, from_sib = self.part, self.from_sib

        def body(rs):
            total = part[k, rs, :].astype(F32) + from_sib[k, rs, :].astype(F32)
            if extra is not None:
                total = total + extra[rs, :].astype(F32)
            part[k, rs, :] = total.astype(BF16)

        _add_rows(self.rows, body)

    def send_direct(self):
        self.swap[1].wait_recv()
        self._fold(1)
        for copy in self.d:
            copy.start()

    def send_chain(self):
        self.swap[2].wait_recv()
        self._fold(2)
        for copy in self.c:
            copy.start()

    def forward_chain(self):
        self.swap[3].wait_recv()
        for copy in self.c:
            copy.wait_recv()
        self._fold(3, self.chain)
        for copy in self.l:
            copy.start()

    def finish(self, o_ref, x_ref):
        self.swap[0].wait_recv()
        for copy in self.d + self.l:
            copy.wait_recv()
        part, from_sib, direct, last = self.part, self.from_sib, self.direct, self.last

        def body(rs):
            total = part[0, rs, :].astype(F32) + from_sib[0, rs, :].astype(F32)
            total = total + direct[rs, :].astype(F32) + last[rs, :].astype(F32)
            o_ref[rs, :] = (x_ref[rs, :].astype(F32) + total.astype(BF16).astype(F32)).astype(BF16)

        _add_rows(self.rows, body)
        for copy in self.swap + self.d + self.c + self.l:
            copy.wait_send()


def _scatter_scratch(rows, model):
    return [
        pltpu.VMEM((4, 2 * rows, model), BF16),
        pltpu.VMEM((4, rows, model), BF16),
        pltpu.VMEM((rows, model), BF16),
        pltpu.VMEM((rows, model), BF16),
        pltpu.VMEM((rows, model), BF16),
        pltpu.SemaphoreType.DMA((10,)),
        pltpu.SemaphoreType.DMA((10,)),
    ]


def _params(collective_id):
    return pltpu.CompilerParams(collective_id=collective_id, has_side_effects=True, vmem_limit_bytes=VMEM_LIMIT)


def _block_kernel(layer, m_hbm, x_ref, g_ref, wo_hbm, wg_hbm, wu_hbm, wd_hbm, o_ref, wo, lhs, buf, wgu, wd, act,
                  part, from_sib, direct, chain, last, s_send, s_recv, o_send, o_recv, g_send, g_recv, w_sem):
    rows, model = x_ref.shape
    half = rows // 2
    cols = act.shape[1]
    x, c, right, left, sib = _place()
    peers = (("tp", left), ("tp", right), ("tp", sib))
    _greet(peers)
    loads = [
        pltpu.make_async_copy(wo_hbm.at[layer], wo, w_sem.at[0]),
        pltpu.make_async_copy(wg_hbm.at[layer], wgu.at[:, pl.ds(0, cols)], w_sem.at[1]),
        pltpu.make_async_copy(wu_hbm.at[layer], wgu.at[:, pl.ds(cols, cols)], w_sem.at[2]),
        pltpu.make_async_copy(wd_hbm.at[layer], wd, w_sem.at[3]),
    ]
    loads[0].start()
    order = (2, 1, 3, 0)
    for k in order:
        for j in range(4):
            start = pl.multiple_of(_piece_rows(x, c, rows, k, j), half)
            pltpu.make_async_copy(m_hbm.at[pl.ds(start, half)], lhs.at[k, pl.ds(j * half, half)], w_sem.at[4 + k]).start()
    for load in loads[1:]:
        load.start()
    buffers = (part, from_sib, direct, chain, last)
    scatter = _Scatter(*buffers, (o_send, o_recv), rows, right, left, sib)
    loads[0].wait()
    for k in order:
        pltpu.make_async_copy(m_hbm.at[pl.ds(0, 2 * rows)], lhs.at[k], w_sem.at[4 + k]).wait()

        def project(n, inner):
            cs = pl.ds(pl.multiple_of(n * OUT_TILE, OUT_TILE), OUT_TILE)
            part[k, :, cs] = jnp.dot(lhs[k], wo[:, cs], preferred_element_type=F32).astype(BF16)
            return inner

        lax.fori_loop(0, model // OUT_TILE, project, 0)
        if k == order[0]:
            _meet(peers)
        scatter.swap[k].start()
        if k == 2:
            scatter.send_chain()
        if k == 1:
            scatter.send_direct()
    scatter.forward_chain()
    scatter.finish(o_ref, x_ref)

    _norm_into(buf, o_ref, g_ref)
    gather = _gather_copies(buf, (g_send, g_recv), rows, right, left, sib)
    _gather_begin(gather)
    scatter = _Scatter(*buffers, (s_send, s_recv), rows, right, left, sib)
    for load in loads[1:]:
        load.wait()

    def step(k, carry):
        for kk in range(4):
            @pl.when(k == kk)
            def _():
                _gather_arrive(kk, gather)
                _relay_arrive(kk, gather)

        def up(n, inner):
            cs = pl.ds(pl.multiple_of(n * UP_TILE, UP_TILE), UP_TILE)
            us = pl.ds(pl.multiple_of(cols + n * UP_TILE, UP_TILE), UP_TILE)
            gate = jnp.dot(buf[k], wgu[:, cs], preferred_element_type=F32)
            lin = jnp.dot(buf[k], wgu[:, us], preferred_element_type=F32)
            act[:, cs] = (jax.nn.silu(gate) * lin).astype(BF16)
            return inner

        lax.fori_loop(0, cols // UP_TILE, up, 0)

        def down(n, inner):
            cs = pl.ds(pl.multiple_of(n * DOWN_TILE, DOWN_TILE), DOWN_TILE)
            part[k, :, cs] = jnp.dot(act[...], wd[:, cs], preferred_element_type=F32).astype(BF16)
            return inner

        lax.fori_loop(0, model // DOWN_TILE, down, 0)
        for kk in range(4):
            @pl.when(k == kk)
            def _():
                scatter.swap[kk].start()
                if kk == 1:
                    scatter.send_direct()
                if kk == 2:
                    scatter.send_chain()
        return carry

    lax.fori_loop(0, 4, step, 0)
    scatter.forward_chain()
    scatter.finish(o_ref, o_ref)
    _gather_end(*gather)


def _block(layer, mixed, x, gain, w_o, w_gate, w_up, w_down):
    rows, model = x.shape
    hd, cols = mixed.shape[1], w_gate.shape[2]
    vmem, hbm = pl.BlockSpec(memory_space=pltpu.VMEM), pl.BlockSpec(memory_space=pl.ANY)
    dma = pltpu.SemaphoreType.DMA
    return pl.pallas_call(
        functools.partial(_block_kernel, layer),
        name=f"block_{layer}",
        out_shape=jax.ShapeDtypeStruct((rows, model), BF16),
        in_specs=[hbm, vmem, vmem, hbm, hbm, hbm, hbm],
        out_specs=vmem,
        scratch_shapes=[
            pltpu.VMEM((hd, model), BF16),
            pltpu.VMEM((4, 2 * rows, hd), BF16),
            pltpu.VMEM((4, 2 * rows, model), BF16),
            pltpu.VMEM((model, 2 * cols), BF16),
            pltpu.VMEM((cols, model), BF16),
            pltpu.VMEM((2 * rows, cols), BF16),
            *_scatter_scratch(rows, model),
            dma((10,)), dma((10,)), dma((12,)), dma((12,)), dma((8,)),
        ],
        compiler_params=_params(layer),
    )(mixed, x, gain, w_o, w_gate, w_up, w_down)


def _qkv_kernel(layer, gather_tab, windowed, shards, x_ref, g_ref, tab_in, wq_hbm, wkv_hbm, *rest):
    if gather_tab:
        n_ref, q_out, kv_out, tab_out, n_out = rest[:5]
        n_y, n_x, n_send, n_recv, c_send, c_recv = rest[5:11]
        rest = rest[11:]
    else:
        q_out, kv_out = rest[:2]
        rest = rest[2:]
    buf, tab, wq, wkv, qs, kv, g_send, g_recv, t_send, t_recv, y_send, y_recv, p_send, p_recv, l_sem, q_sem, w_sem = rest
    rows, model = x_ref.shape
    half, step_rows = rows // 2, 2 * rows
    shard = 4 * step_rows
    hd = wq.shape[1]
    x, c, right, left, sib = _place()
    y = lax.axis_index("sp")
    up, down = lax.rem(y + 1, shards), lax.rem(y + shards - 1, shards)
    peers = (("tp", left), ("tp", right), ("tp", sib), ("sp", up), ("sp", down))
    _greet(peers)
    loads = [pltpu.make_async_copy(wq_hbm.at[layer], wq, w_sem.at[0]), pltpu.make_async_copy(wkv_hbm.at[layer], wkv, w_sem.at[1])]
    for load in loads:
        load.start()
    if not gather_tab:
        tab_load = pltpu.make_async_copy(tab_in, tab, w_sem.at[2])
        tab_load.start()
    else:
        tab_load = pltpu.make_async_copy(tab_in, tab.at[0, pl.ds(0, rows)], w_sem.at[2])
        tab_load.start()
    _norm_into(buf, x_ref, g_ref)
    if gather_tab:
        n_y[0] = n_ref[...]
    tab_load.wait()
    _meet(peers)
    gather = _gather_copies(buf, (g_send, g_recv), rows, right, left, sib)
    gathers = [gather]
    if gather_tab:
        gathers.insert(0, _gather_copies(tab, (t_send, t_recv), rows, right, left, sib))
        n_copies = [_copy(n_y.at[src], n_y.at[dst], (c_send, c_recv), i, "sp", dev) for i, (src, dst, dev) in enumerate(((0, 1, up), (0, 2, down), (1, 3, up)))]
        n_copies[0].start()
        n_copies[1].start()
    _gather_begin(*gathers)
    if gather_tab:
        n_copies[0].wait_recv()
        n_copies[2].start()
        n_copies[1].wait_recv()
        n_copies[2].wait_recv()
        n_x[0, :32, :] = jnp.zeros((32, 128), F32)
        n_x[0, :8, :] = n_y[0] + n_y[1] + n_y[2] + n_y[3]
        gathers.append(_gather_copies(n_x, (n_send, n_recv), 32, right, left, sib))
        _gather_begin(gathers[2])

    if windowed:
        bases = (shard, 0)
    else:
        bases = tuple(lax.rem(y + d, shards) * shard for d in (0, shards - 1, 1, 2))

    def y_copies(k):
        a, b = pl.ds(k * step_rows, rows), pl.ds(k * step_rows + rows, rows)
        sems = (y_send, y_recv)
        first, second = [], []
        for i, part in enumerate((a, b)):
            first.append([_copy(kv.at[0, part], kv.at[1, part], sems, 6 * k + 2 * i, "sp", up)])
            if not windowed:
                first[i].append(_copy(kv.at[0, part], kv.at[2, part], sems, 6 * k + 2 * i + 1, "sp", down))
        if not windowed:
            second.append(_copy(kv.at[1, a], kv.at[3, a], sems, 6 * k + 4, "sp", up))
            second.append(_copy(kv.at[2, b], kv.at[3, b], sems, 6 * k + 5, "sp", down))
        return first, second

    def place(s, k, js=range(4)):
        for j in js:
            src = kv.at[s, pl.ds(k * step_rows + j * half, half)]
            start = pl.multiple_of(bases[s] + _piece_rows(x, c, rows, k, j), half)
            dst = kv_out.at[c, pl.ds(start, half)]
            pltpu.make_async_copy(src, dst, l_sem.at[s]).start()
            _copy(src, dst, (p_send, p_recv), s, "tp", sib).start()

    def forward(k):
        first, second = y_copies(k)
        first[0][0].wait_recv()
        if not windowed:
            second[0].start()
        first[1][0].wait_recv()
        if not windowed:
            first[1][1].wait_recv()
            second[1].start()
            first[0][1].wait_recv()
            place(2, k)
        place(1, k)

    def opposite(k):
        first, second = y_copies(k)
        for copy in second:
            copy.wait_recv()
        if second:
            place(3, k)

    def step(k, carry):
        for kk in range(4):
            @pl.when(k == kk)
            def _():
                if kk == 0:
                    loads[0].wait()
                    loads[1].wait()
                _gather_arrive(kk, *gathers)

        def part(h, inner):
            for kk in range(4):
                @pl.when((k == kk) & (h == 1))
                def _():
                    _relay_arrive(kk, *gathers)

            ps = pl.ds(pl.multiple_of(h * rows, rows), rows)
            rs = pl.ds(pl.multiple_of(k * step_rows + h * rows, rows), rows)
            cos, sin = tab[k, ps, :hd // 2], tab[k, ps, hd // 2:]

            def rotate(t):
                lower, upper = t[:, :hd // 2], t[:, hd // 2:]
                return jnp.concatenate([lower * cos - upper * sin, upper * cos + lower * sin], axis=-1).astype(BF16)

            t = jnp.dot(buf[k, ps, :], wkv[...], preferred_element_type=F32).astype(BF16)

            @pl.when(c == 0)
            def _():
                kv[0, rs, :] = rotate(t.astype(F32))

            @pl.when(c == 1)
            def _():
                kv[0, rs, :] = t

            for kk in range(4):
                for hh in range(2):
                    @pl.when((k == kk) & (h == hh))
                    def _():
                        for copy in y_copies(kk)[0][hh]:
                            copy.start()
                        place(0, kk, (2 * hh, 2 * hh + 1))

            q = jnp.dot(buf[k, ps, :], wq[...], preferred_element_type=F32).astype(BF16).astype(F32)
            qs[rs, :] = rotate(q)
            return inner

        lax.fori_loop(0, 2, part, 0)
        for kk in range(4):
            @pl.when(k == kk)
            def _():
                for j in range(4):
                    start = pl.multiple_of(_piece_rows(x, c, rows, kk, j), half)
                    pltpu.make_async_copy(qs.at[pl.ds(kk * step_rows + j * half, half)], q_out.at[pl.ds(start, half)], q_sem.at[0]).start()
                if kk >= 1:
                    forward(kk - 1)
                if kk >= 2:
                    opposite(kk - 2)
        return carry

    lax.fori_loop(0, 4, step, 0)
    forward(3)
    opposite(2)
    opposite(3)
    if gather_tab:
        store = pltpu.make_async_copy(tab, tab_out, w_sem.at[3])
        store.start()
        store.wait()
        total = n_x[0, :8, :]
        for k in range(4):
            for i in range(8):
                if k or i:
                    total = total + n_x[k, 8 * i:8 * i + 8, :]
        n_out[...] = total
        for copy in n_copies:
            copy.wait_send()
    pltpu.make_async_copy(qs, q_out, q_sem.at[0]).wait()
    for s, base in enumerate(bases):
        span = pl.ds(pl.multiple_of(base, shard), shard)
        pltpu.make_async_copy(kv.at[s], kv_out.at[c, span], l_sem.at[s]).wait()
        swap = _copy(kv.at[s], kv_out.at[c, span], (p_send, p_recv), s, "tp", sib)
        swap.wait_send()
        swap.wait_recv()
    for k in range(4):
        first, second = y_copies(k)
        for copy in first[0] + first[1] + second:
            copy.wait_send()
    for ring, relay in gathers:
        _gather_end(ring, relay)


def _qkv(layer, windowed, shards, x, gain, tab, w_q, w_kv, counts):
    rows, model = x.shape
    hd = w_q.shape[2]
    gather_tab = tab.ndim == 2
    shard = 8 * rows
    held = 2 if windowed else shards
    vmem, hbm = pl.BlockSpec(memory_space=pltpu.VMEM), pl.BlockSpec(memory_space=pl.ANY)
    tab_shape = (4, 2 * rows, hd)
    out_shape = [jax.ShapeDtypeStruct((shard, hd), BF16), jax.ShapeDtypeStruct((2, held * shard, hd), BF16)]
    if gather_tab:
        out_shape += [jax.ShapeDtypeStruct(tab_shape, F32), jax.ShapeDtypeStruct(counts.shape, F32)]
    dma = pltpu.SemaphoreType.DMA
    count_scratch = [pltpu.VMEM((4, *counts.shape), F32), pltpu.VMEM((4, 64, 128), F32), dma((12,)), dma((12,)), dma((3,)), dma((3,))]
    return pl.pallas_call(
        functools.partial(_qkv_kernel, layer, gather_tab, windowed, shards),
        name=f"qkv_{layer}",
        out_shape=out_shape,
        in_specs=[vmem, vmem, hbm, hbm, hbm] + [vmem] * gather_tab,
        out_specs=[hbm] * 3 + [vmem] if gather_tab else [hbm] * 2,
        scratch_shapes=[
            *(count_scratch if gather_tab else []),
            pltpu.VMEM((4, 2 * rows, model), BF16),
            pltpu.VMEM(tab_shape, F32),
            pltpu.VMEM((model, hd), BF16),
            pltpu.VMEM((model, hd), BF16),
            pltpu.VMEM((shard, hd), BF16),
            pltpu.VMEM((held, shard, hd), BF16),
            pltpu.SemaphoreType.DMA((12,)),
            pltpu.SemaphoreType.DMA((12,)),
            pltpu.SemaphoreType.DMA((12,)),
            pltpu.SemaphoreType.DMA((12,)),
            pltpu.SemaphoreType.DMA((24,)),
            pltpu.SemaphoreType.DMA((24,)),
            pltpu.SemaphoreType.DMA((4,)),
            pltpu.SemaphoreType.DMA((4,)),
            pltpu.SemaphoreType.DMA((4,)),
            pltpu.SemaphoreType.DMA((1,)),
            pltpu.SemaphoreType.DMA((4,)),
        ],
        compiler_params=_params(4 + layer),
    )(x, gain, tab, w_q, w_kv, *([counts] if gather_tab else []))


def _attend_kernel(scale, k_block, bounds, q_ref, lo_ref, kv_ref, o_ref, m_sc, l_sc, acc_sc):
    i = pl.program_id(0)
    rows, hd = q_ref.shape
    m_sc[...] = jnp.full(m_sc.shape, -1e30, F32)
    l_sc[...] = jnp.zeros(l_sc.shape, F32)
    acc_sc[...] = jnp.zeros(acc_sc.shape, F32)
    first = bounds[4, i]

    def block(masked, b, carry):
        start = pl.multiple_of(b * k_block, k_block)
        k = kv_ref[0, pl.ds(start, k_block), :]
        v = kv_ref[1, pl.ds(start, k_block), :]
        s = lax.dot_general(k, q_ref[...], (((1,), (1,)), ((), ())), preferred_element_type=F32)
        if masked:
            j = start + lax.broadcasted_iota(jnp.int32, (k_block, rows), 0)
            r = first + lax.broadcasted_iota(jnp.int32, (k_block, rows), 1)
            s = jnp.where((j <= r) & (j >= lo_ref[...]), s, -1e30)
        m_old = m_sc[...]
        m_new = jnp.maximum(m_old, jnp.max(s, axis=0, keepdims=True))
        p = jnp.exp2((s - m_new) * scale)
        alpha = jnp.exp2((m_old - m_new) * scale)
        m_sc[...] = m_new
        l_sc[...] = l_sc[...] * alpha + jnp.sum(p, axis=0, keepdims=True)
        add = lax.dot_general(v, p.astype(BF16), (((0,), (0,)), ((), ())), preferred_element_type=F32)
        acc_sc[...] = acc_sc[...] * alpha + add
        return carry

    lax.fori_loop(bounds[0, i], bounds[1, i], functools.partial(block, True), 0)
    lax.fori_loop(bounds[1, i], bounds[2, i], functools.partial(block, False), 0)
    lax.fori_loop(bounds[2, i], bounds[3, i], functools.partial(block, True), 0)
    o_ref[...] = jnp.transpose(acc_sc[...] / l_sc[...]).astype(BF16)


def _attend(q, kv, row_lo, first_row, block):
    total, hd = q.shape
    blocks = total // block
    lo2 = row_lo.reshape(blocks, block)
    first = first_row + jnp.arange(blocks, dtype=jnp.int32) * block
    b_lo = lo2[:, 0] // block
    b_hi = (first + block - 1) // block + 1
    b_a = jnp.clip((lo2[:, -1] + block - 1) // block, b_lo, b_hi)
    b_b = jnp.clip((first + 1) // block, b_a, b_hi)
    bounds = jnp.stack([b_lo, b_a, b_b, b_hi, first]).astype(jnp.int32)
    return pl.pallas_call(
        functools.partial(_attend_kernel, hd ** -0.5 * math.log2(math.e), block),
        name="attend",
        out_shape=jax.ShapeDtypeStruct((total, hd), BF16),
        grid_spec=pltpu.PrefetchScalarGridSpec(
            num_scalar_prefetch=1,
            grid=(blocks,),
            in_specs=[
                pl.BlockSpec((block, hd), lambda i, b: (i, 0)),
                pl.BlockSpec((1, block), lambda i, b: (0, i)),
                pl.BlockSpec(memory_space=pltpu.VMEM),
            ],
            out_specs=pl.BlockSpec((block, hd), lambda i, b: (i, 0)),
            scratch_shapes=[pltpu.VMEM((1, block), F32), pltpu.VMEM((1, block), F32), pltpu.VMEM((hd, block), F32)],
        ),
        compiler_params=pltpu.CompilerParams(dimension_semantics=("arbitrary",), vmem_limit_bytes=VMEM_LIMIT),
    )(bounds, q, row_lo.reshape(1, total), kv)


def solution(mesh):
    tp_size, shards = mesh.shape["tp"], mesh.shape["sp"]
    row_spec = P(("dp", "sp", "tp"), None)
    id_spec = P(("dp", "sp", "tp"))
    whole = P()
    in_specs = (row_spec, id_spec, id_spec, whole, P(None, None, "tp", None), whole, whole, P(None, "tp", None, None), whole, P(None, None, "tp"), P(None, None, "tp"), P(None, "tp", None))

    def local_fn(x, segment_ids, positions, g_attn, w_q, w_k, w_v, w_o, g_mlp, w_gate, w_up, w_down):
        sp_idx = lax.axis_index("sp")
        tp_idx = lax.axis_index("tp")
        layers, model, heads_loc, hd = w_q.shape
        rows = x.shape[0]
        shard = rows * tp_size
        kv_head = tp_idx * w_k.shape[2] // tp_size
        inv_freq = ROPE_BASE ** (-jnp.arange(hd // 2, dtype=F32) / (hd // 2))
        angles = positions.astype(F32)[:, None] * inv_freq[None, :]
        tab = jnp.concatenate([jnp.cos(angles), jnp.sin(angles)], axis=1)
        lane = lax.broadcasted_iota(jnp.int32, (8, 128), 1)
        counts = jnp.where(lane == 0, jnp.sum(segment_ids < 1), jnp.where(lane == 1, jnp.sum(segment_ids < 2), 0)).astype(F32)
        token = sp_idx * shard + jnp.arange(shard, dtype=jnp.int32)


        def pick(w):
            return lax.optimization_barrier(lax.dynamic_slice_in_dim(w, kv_head, 1, 2).reshape(layers, model, hd))

        w_kv = lax.cond(tp_idx % 2 == 0, lambda: pick(w_k), lambda: pick(w_v))
        w_q2 = w_q.reshape(layers, model, hd)
        w_o2 = w_o.reshape(layers, hd, model)
        for layer in range(layers):
            windowed = layer % 2 == 0
            got = _qkv(layer, windowed, shards, x, g_attn[layer:layer + 1], tab, w_q2, w_kv, counts)
            q, kv = got[0], got[1]
            if layer == 0:
                tab = got[2]
                second, third = got[3][0, 0].astype(jnp.int32), got[3][0, 1].astype(jnp.int32)
                seg_lo = jnp.where(token >= third, third, jnp.where(token >= second, second, 0))
            if windowed:
                shift = (sp_idx - 1) * shard
                row_lo = jnp.maximum(seg_lo, token - (WINDOW - 1)) - shift
            else:
                shift = 0
                row_lo = seg_lo
            mixed = _attend(q, kv, row_lo, sp_idx * shard - shift, 512 if windowed else 1024)
            x = _block(layer, mixed, x, g_mlp[layer:layer + 1], w_o2, w_gate, w_up, w_down)
        return x

    return jax.shard_map(local_fn, mesh=mesh, in_specs=in_specs, out_specs=row_spec, check_vma=False)
```

```python
import functools
import math

import jax
import jax.numpy as jnp
from jax import lax
from jax.experimental import pallas as pl
from jax.experimental.pallas import tpu as pltpu
from jax.sharding import PartitionSpec as P

EPS = 1e-6
ROPE_BASE = 10000.0
WINDOW = 1024
CHIPS = 4
MESH = pl.DeviceIdType.MESH
BF16 = jnp.bfloat16
F32 = jnp.float32
VMEM_LIMIT = 66_000_000
UP_TILE = 1280
DOWN_TILE = 1280
OUT_TILE = 1280


def _place():
    t = lax.axis_index("tp")
    c = lax.rem(t, 2)
    x = t // 2
    right = lax.rem(x + 1, CHIPS) * 2 + c
    left = lax.rem(x + CHIPS - 1, CHIPS) * 2 + c
    sib = x * 2 + 1 - c
    return x, c, right, left, sib


def _copy(src, dst, sems, index, axis, dev):
    send, recv = sems
    return pltpu.make_async_remote_copy(
        src_ref=src, dst_ref=dst, send_sem=send.at[index], recv_sem=recv.at[index],
        device_id={axis: dev}, device_id_type=MESH)


def _greet(peers):
    bar = pltpu.get_barrier_semaphore()
    for axis, dev in peers:
        pl.semaphore_signal(bar, inc=1, device_id={axis: dev}, device_id_type=MESH)


def _meet(peers):
    pl.semaphore_wait(pltpu.get_barrier_semaphore(), len(peers))


def _piece_rows(x, c, rows, k, j):
    half = rows // 2
    core = c if j < 2 else 1 - c
    even = j % 2 == 0
    if k == 0:
        chip, h = x, j % 2
    elif k == 1:
        chip, h = (x + CHIPS - 1, 0) if even else (x + 1, 1)
    elif k == 2:
        chip, h = x + 2, j % 2
    else:
        chip, h = (x + CHIPS - 1, 1) if even else (x + 1, 0)
    return lax.rem(chip, CHIPS) * (2 * rows) + core * rows + h * half


def _gather_copies(buf, sems, rows, right, left, sib):
    half, part = rows // 2, rows // 4
    a, b = pl.ds(0, half), pl.ds(half, half)
    a1, a2, b1, b2 = (pl.ds(i * part, part) for i in range(4))
    ring = [
        _copy(buf.at[0, a], buf.at[1, a], sems, 0, "tp", right),
        _copy(buf.at[0, b], buf.at[1, b], sems, 1, "tp", left),
        _copy(buf.at[0, b1], buf.at[3, a1], sems, 2, "tp", right),
        _copy(buf.at[0, a1], buf.at[3, b1], sems, 3, "tp", left),
        _copy(buf.at[1, a], buf.at[2, a], sems, 4, "tp", right),
        _copy(buf.at[1, b], buf.at[2, b], sems, 5, "tp", left),
        _copy(buf.at[0, b2], buf.at[3, a2], sems, 6, "tp", right),
        _copy(buf.at[0, a2], buf.at[3, b2], sems, 7, "tp", left),
    ]
    relay = [_copy(buf.at[k, pl.ds(0, rows)], buf.at[k, pl.ds(rows, rows)], sems, 8 + k, "tp", sib) for k in range(4)]
    return ring, relay


def _gather_begin(*gathers):
    for i in (0, 1):
        for ring, relay in gathers:
            ring[i].start()
    for ring, relay in gathers:
        relay[0].start()
    for i in (2, 3):
        for ring, relay in gathers:
            ring[i].start()


def _gather_arrive(k, *gathers):
    if k == 1:
        for i in (0, 1):
            for ring, relay in gathers:
                ring[i].wait_recv()
                ring[4 + i].start()
        for i in (6, 7):
            for ring, relay in gathers:
                ring[i].start()
    for ring, relay in gathers:
        for i in {2: (4, 5), 3: (2, 3, 6, 7)}.get(k, ()):
            ring[i].wait_recv()
        if k >= 1:
            relay[k].start()


def _relay_arrive(k, *gathers):
    for ring, relay in gathers:
        relay[k].wait_recv()


def _gather_end(ring, relay):
    for copy in ring + relay:
        copy.wait_send()


def _norm_into(dst, x_ref, g_ref, layer):
    rows = x_ref.shape[0]
    gain = g_ref[layer:layer + 1, :].astype(F32)
    chunk = 16

    def body(i, carry):
        rs = pl.ds(pl.multiple_of(i * chunk, chunk), chunk)
        wide = x_ref[rs, :].astype(F32)
        inv = lax.rsqrt(jnp.mean(wide * wide, axis=-1, keepdims=True) + EPS)
        dst[0, rs, :] = (wide * inv * gain).astype(BF16)
        return carry

    lax.fori_loop(0, rows // chunk, body, 0)


def _add_rows(rows, body):
    chunk = 16

    def step(i, carry):
        body(pl.ds(pl.multiple_of(i * chunk, chunk), chunk))
        return carry

    lax.fori_loop(0, rows // chunk, step, 0)


class _Scatter:
    def __init__(self, part, from_sib, direct, chain, last, sems, rows, right, left, sib):
        half = rows // 2
        a, b = pl.ds(0, half), pl.ds(half, half)
        self.rows, self.part, self.from_sib = rows, part, from_sib
        self.direct, self.chain, self.last = direct, chain, last
        self.swap = [_copy(part.at[k, pl.ds(rows, rows)], from_sib.at[k], sems, k, "tp", sib) for k in range(4)]
        self.d = [_copy(part.at[1, b], direct.at[b], sems, 4, "tp", right), _copy(part.at[1, a], direct.at[a], sems, 5, "tp", left)]
        self.c = [_copy(part.at[2, a], chain.at[b], sems, 6, "tp", right), _copy(part.at[2, b], chain.at[a], sems, 7, "tp", left)]
        self.l = [_copy(part.at[3, b], last.at[a], sems, 8, "tp", right), _copy(part.at[3, a], last.at[b], sems, 9, "tp", left)]

    def _fold(self, k, extra=None):
        part, from_sib = self.part, self.from_sib

        def body(rs):
            total = part[k, rs, :].astype(F32) + from_sib[k, rs, :].astype(F32)
            if extra is not None:
                total = total + extra[rs, :].astype(F32)
            part[k, rs, :] = total.astype(BF16)

        _add_rows(self.rows, body)

    def send_direct(self):
        self.swap[1].wait_recv()
        self._fold(1)
        for copy in self.d:
            copy.start()

    def send_chain(self):
        self.swap[2].wait_recv()
        self._fold(2)
        for copy in self.c:
            copy.start()

    def forward_chain(self):
        self.swap[3].wait_recv()
        for copy in self.c:
            copy.wait_recv()
        self._fold(3, self.chain)
        for copy in self.l:
            copy.start()

    def finish(self, o_ref, x_ref):
        self.swap[0].wait_recv()
        for copy in self.d + self.l:
            copy.wait_recv()
        part, from_sib, direct, last = self.part, self.from_sib, self.direct, self.last

        def body(rs):
            total = part[0, rs, :].astype(F32) + from_sib[0, rs, :].astype(F32)
            total = total + direct[rs, :].astype(F32) + last[rs, :].astype(F32)
            o_ref[rs, :] = (x_ref[rs, :].astype(F32) + total.astype(BF16).astype(F32)).astype(BF16)

        _add_rows(self.rows, body)
        for copy in self.swap + self.d + self.c + self.l:
            copy.wait_send()


def _scatter_scratch(rows, model):
    return [
        pltpu.VMEM((4, 2 * rows, model), BF16),
        pltpu.VMEM((4, rows, model), BF16),
        pltpu.VMEM((rows, model), BF16),
        pltpu.VMEM((rows, model), BF16),
        pltpu.VMEM((rows, model), BF16),
        pltpu.SemaphoreType.DMA((10,)),
        pltpu.SemaphoreType.DMA((10,)),
    ]


def _params(collective_id):
    return pltpu.CompilerParams(collective_id=collective_id, has_side_effects=True, vmem_limit_bytes=VMEM_LIMIT)


def _block_kernel(layer, m_hbm, x_ref, g_ref, wo_hbm, wg_hbm, wu_hbm, wd_hbm, o_ref, wo, lhs, buf, wgu, wd, act,
                  part, from_sib, direct, chain, last, s_send, s_recv, o_send, o_recv, g_send, g_recv, w_sem):
    rows, model = x_ref.shape
    half = rows // 2
    cols = act.shape[1]
    x, c, right, left, sib = _place()
    peers = (("tp", left), ("tp", right), ("tp", sib))
    _greet(peers)
    loads = [
        pltpu.make_async_copy(wo_hbm.at[layer], wo, w_sem.at[0]),
        pltpu.make_async_copy(wg_hbm.at[layer], wgu.at[:, pl.ds(0, cols)], w_sem.at[1]),
        pltpu.make_async_copy(wu_hbm.at[layer], wgu.at[:, pl.ds(cols, cols)], w_sem.at[2]),
        pltpu.make_async_copy(wd_hbm.at[layer], wd, w_sem.at[3]),
    ]
    loads[0].start()
    order = (2, 1, 3, 0)
    for k in order:
        for j in range(4):
            start = pl.multiple_of(_piece_rows(x, c, rows, k, j), half)
            pltpu.make_async_copy(m_hbm.at[pl.ds(start, half)], lhs.at[k, pl.ds(j * half, half)], w_sem.at[4 + k]).start()
    for load in loads[1:]:
        load.start()
    buffers = (part, from_sib, direct, chain, last)
    scatter = _Scatter(*buffers, (o_send, o_recv), rows, right, left, sib)
    loads[0].wait()
    for k in order:
        pltpu.make_async_copy(m_hbm.at[pl.ds(0, 2 * rows)], lhs.at[k], w_sem.at[4 + k]).wait()

        def project(n, inner):
            cs = pl.ds(pl.multiple_of(n * OUT_TILE, OUT_TILE), OUT_TILE)
            part[k, :, cs] = jnp.dot(lhs[k], wo[:, cs], preferred_element_type=F32).astype(BF16)
            return inner

        lax.fori_loop(0, model // OUT_TILE, project, 0)
        if k == order[0]:
            _meet(peers)
        scatter.swap[k].start()
        if k == 2:
            scatter.send_chain()
        if k == 1:
            scatter.send_direct()
    scatter.forward_chain()
    scatter.finish(o_ref, x_ref)

    _norm_into(buf, o_ref, g_ref, layer)
    gather = _gather_copies(buf, (g_send, g_recv), rows, right, left, sib)
    _gather_begin(gather)
    scatter = _Scatter(*buffers, (s_send, s_recv), rows, right, left, sib)
    for load in loads[1:]:
        load.wait()

    def step(k, carry):
        for kk in range(4):
            @pl.when(k == kk)
            def _():
                _gather_arrive(kk, gather)
                _relay_arrive(kk, gather)

        def up(n, inner):
            cs = pl.ds(pl.multiple_of(n * UP_TILE, UP_TILE), UP_TILE)
            us = pl.ds(pl.multiple_of(cols + n * UP_TILE, UP_TILE), UP_TILE)
            gate = jnp.dot(buf[k], wgu[:, cs], preferred_element_type=F32)
            lin = jnp.dot(buf[k], wgu[:, us], preferred_element_type=F32)
            act[:, cs] = (jax.nn.silu(gate) * lin).astype(BF16)
            return inner

        lax.fori_loop(0, cols // UP_TILE, up, 0)

        def down(n, inner):
            cs = pl.ds(pl.multiple_of(n * DOWN_TILE, DOWN_TILE), DOWN_TILE)
            part[k, :, cs] = jnp.dot(act[...], wd[:, cs], preferred_element_type=F32).astype(BF16)
            return inner

        lax.fori_loop(0, model // DOWN_TILE, down, 0)
        for kk in range(4):
            @pl.when(k == kk)
            def _():
                scatter.swap[kk].start()
                if kk == 1:
                    scatter.send_direct()
                if kk == 2:
                    scatter.send_chain()
        return carry

    lax.fori_loop(0, 4, step, 0)
    scatter.forward_chain()
    scatter.finish(o_ref, o_ref)
    _gather_end(*gather)


def _block(layer, mixed, x, gain, w_o, w_gate, w_up, w_down):
    rows, model = x.shape
    hd, cols = mixed.shape[1], w_gate.shape[2]
    vmem, hbm = pl.BlockSpec(memory_space=pltpu.VMEM), pl.BlockSpec(memory_space=pl.ANY)
    dma = pltpu.SemaphoreType.DMA
    return pl.pallas_call(
        functools.partial(_block_kernel, layer),
        name=f"block_{layer}",
        out_shape=jax.ShapeDtypeStruct((rows, model), BF16),
        in_specs=[hbm, vmem, vmem, hbm, hbm, hbm, hbm],
        out_specs=vmem,
        scratch_shapes=[
            pltpu.VMEM((hd, model), BF16),
            pltpu.VMEM((4, 2 * rows, hd), BF16),
            pltpu.VMEM((4, 2 * rows, model), BF16),
            pltpu.VMEM((model, 2 * cols), BF16),
            pltpu.VMEM((cols, model), BF16),
            pltpu.VMEM((2 * rows, cols), BF16),
            *_scatter_scratch(rows, model),
            dma((10,)), dma((10,)), dma((12,)), dma((12,)), dma((8,)),
        ],
        compiler_params=_params(layer),
    )(mixed, x, gain, w_o, w_gate, w_up, w_down)


def _qkv_kernel(layer, gather_tab, windowed, shards, x_ref, g_ref, tab_in, wq_hbm, wkv_hbm, *rest):
    if gather_tab:
        n_ref, q_out, kv_out, tab_out, n_out = rest[:5]
        n_y, n_x, n_send, n_recv, c_send, c_recv = rest[5:11]
        rest = rest[11:]
    else:
        q_out, kv_out = rest[:2]
        rest = rest[2:]
    buf, tab, wq, wkv, qs, kv, g_send, g_recv, t_send, t_recv, y_send, y_recv, p_send, p_recv, l_sem, q_sem, w_sem = rest
    rows, model = x_ref.shape
    half, step_rows = rows // 2, 2 * rows
    shard = 4 * step_rows
    hd = wq.shape[1]
    x, c, right, left, sib = _place()
    y = lax.axis_index("sp")
    up, down = lax.rem(y + 1, shards), lax.rem(y + shards - 1, shards)
    peers = (("tp", left), ("tp", right), ("tp", sib), ("sp", up), ("sp", down))
    _greet(peers)
    loads = [pltpu.make_async_copy(wq_hbm.at[layer], wq, w_sem.at[0]), pltpu.make_async_copy(wkv_hbm.at[layer], wkv, w_sem.at[1])]
    for load in loads:
        load.start()
    if not gather_tab:
        tab_load = pltpu.make_async_copy(tab_in, tab, w_sem.at[2])
        tab_load.start()
    else:
        tab_load = pltpu.make_async_copy(tab_in, tab.at[0, pl.ds(0, rows)], w_sem.at[2])
        tab_load.start()
    _norm_into(buf, x_ref, g_ref, layer)
    if gather_tab:
        ids = n_ref[...]
        n_y[0] = jnp.zeros(n_y.shape[1:], F32)
        n_y[0, 0:2, :] = jnp.where(ids < 1, 1.0, 0.0)
        n_y[0, 2:4, :] = jnp.where(ids < 2, 1.0, 0.0)
    tab_load.wait()
    _meet(peers)
    gather = _gather_copies(buf, (g_send, g_recv), rows, right, left, sib)
    gathers = [gather]
    if gather_tab:
        gathers.insert(0, _gather_copies(tab, (t_send, t_recv), rows, right, left, sib))
        n_copies = [_copy(n_y.at[src], n_y.at[dst], (c_send, c_recv), i, "sp", dev) for i, (src, dst, dev) in enumerate(((0, 1, up), (0, 2, down), (1, 3, up)))]
        n_copies[0].start()
        n_copies[1].start()
    _gather_begin(*gathers)
    if gather_tab:
        n_copies[0].wait_recv()
        n_copies[2].start()
        n_copies[1].wait_recv()
        n_copies[2].wait_recv()
        n_x[0, :32, :] = jnp.zeros((32, 128), F32)
        n_x[0, :8, :] = n_y[0] + n_y[1] + n_y[2] + n_y[3]
        gathers.append(_gather_copies(n_x, (n_send, n_recv), 32, right, left, sib))
        _gather_begin(gathers[2])

    if windowed:
        bases = (shard, 0)
    else:
        bases = tuple(lax.rem(y + d, shards) * shard for d in (0, shards - 1, 1, 2))

    def y_copies(k):
        a, b = pl.ds(k * step_rows, rows), pl.ds(k * step_rows + rows, rows)
        sems = (y_send, y_recv)
        first, second = [], []
        for i, part in enumerate((a, b)):
            first.append([_copy(kv.at[0, part], kv.at[1, part], sems, 6 * k + 2 * i, "sp", up)])
            if not windowed:
                first[i].append(_copy(kv.at[0, part], kv.at[2, part], sems, 6 * k + 2 * i + 1, "sp", down))
        if not windowed:
            second.append(_copy(kv.at[1, a], kv.at[3, a], sems, 6 * k + 4, "sp", up))
            second.append(_copy(kv.at[2, b], kv.at[3, b], sems, 6 * k + 5, "sp", down))
        return first, second

    def place(s, k, js=range(4)):
        for j in js:
            src = kv.at[s, pl.ds(k * step_rows + j * half, half)]
            start = pl.multiple_of(bases[s] + _piece_rows(x, c, rows, k, j), half)
            dst = kv_out.at[c, pl.ds(start, half)]
            pltpu.make_async_copy(src, dst, l_sem.at[s]).start()
            _copy(src, dst, (p_send, p_recv), s, "tp", sib).start()

    def forward(k):
        first, second = y_copies(k)
        first[0][0].wait_recv()
        if not windowed:
            second[0].start()
        first[1][0].wait_recv()
        if not windowed:
            first[1][1].wait_recv()
            second[1].start()
            first[0][1].wait_recv()
            place(2, k)
        place(1, k)

    def opposite(k):
        first, second = y_copies(k)
        for copy in second:
            copy.wait_recv()
        if second:
            place(3, k)

    def step(k, carry):
        for kk in range(4):
            @pl.when(k == kk)
            def _():
                if kk == 0:
                    loads[0].wait()
                    loads[1].wait()
                _gather_arrive(kk, *gathers)

        def part(h, inner):
            for kk in range(4):
                @pl.when((k == kk) & (h == 1))
                def _():
                    _relay_arrive(kk, *gathers)

            ps = pl.ds(pl.multiple_of(h * rows, rows), rows)
            rs = pl.ds(pl.multiple_of(k * step_rows + h * rows, rows), rows)
            cos, sin = tab[k, ps, :hd // 2], tab[k, ps, hd // 2:]

            def rotate(t):
                lower, upper = t[:, :hd // 2], t[:, hd // 2:]
                return jnp.concatenate([lower * cos - upper * sin, upper * cos + lower * sin], axis=-1).astype(BF16)

            t = jnp.dot(buf[k, ps, :], wkv[...], preferred_element_type=F32).astype(BF16)

            @pl.when(c == 0)
            def _():
                kv[0, rs, :] = rotate(t.astype(F32))

            @pl.when(c == 1)
            def _():
                kv[0, rs, :] = t

            for kk in range(4):
                for hh in range(2):
                    @pl.when((k == kk) & (h == hh))
                    def _():
                        for copy in y_copies(kk)[0][hh]:
                            copy.start()
                        place(0, kk, (2 * hh, 2 * hh + 1))

            q = jnp.dot(buf[k, ps, :], wq[...], preferred_element_type=F32).astype(BF16).astype(F32)
            qs[rs, :] = rotate(q)
            return inner

        lax.fori_loop(0, 2, part, 0)
        for kk in range(4):
            @pl.when(k == kk)
            def _():
                for j in range(4):
                    start = pl.multiple_of(_piece_rows(x, c, rows, kk, j), half)
                    pltpu.make_async_copy(qs.at[pl.ds(kk * step_rows + j * half, half)], q_out.at[pl.ds(start, half)], q_sem.at[0]).start()
                if kk >= 1:
                    forward(kk - 1)
                if kk >= 2:
                    opposite(kk - 2)
        return carry

    lax.fori_loop(0, 4, step, 0)
    forward(3)
    opposite(2)
    opposite(3)
    if gather_tab:
        store = pltpu.make_async_copy(tab, tab_out, w_sem.at[3])
        store.start()
        store.wait()
        total = n_x[0, :8, :]
        for k in range(4):
            for i in range(8):
                if k or i:
                    total = total + n_x[k, 8 * i:8 * i + 8, :]
        n_out[...] = total
        for copy in n_copies:
            copy.wait_send()
    pltpu.make_async_copy(qs, q_out, q_sem.at[0]).wait()
    for s, base in enumerate(bases):
        span = pl.ds(pl.multiple_of(base, shard), shard)
        pltpu.make_async_copy(kv.at[s], kv_out.at[c, span], l_sem.at[s]).wait()
        swap = _copy(kv.at[s], kv_out.at[c, span], (p_send, p_recv), s, "tp", sib)
        swap.wait_send()
        swap.wait_recv()
    for k in range(4):
        first, second = y_copies(k)
        for copy in first[0] + first[1] + second:
            copy.wait_send()
    for ring, relay in gathers:
        _gather_end(ring, relay)


def _qkv(layer, windowed, shards, x, gain, tab, w_q, w_kv, counts):
    rows, model = x.shape
    hd = w_q.shape[2]
    gather_tab = tab.ndim == 2
    shard = 8 * rows
    held = 2 if windowed else shards
    vmem, hbm = pl.BlockSpec(memory_space=pltpu.VMEM), pl.BlockSpec(memory_space=pl.ANY)
    tab_shape = (4, 2 * rows, hd)
    out_shape = [jax.ShapeDtypeStruct((shard, hd), BF16), jax.ShapeDtypeStruct((2, held * shard, hd), BF16)]
    if gather_tab:
        out_shape += [jax.ShapeDtypeStruct(tab_shape, F32), jax.ShapeDtypeStruct((8, 128), F32)]
    dma = pltpu.SemaphoreType.DMA
    count_scratch = [pltpu.VMEM((4, 8, 128), F32), pltpu.VMEM((4, 64, 128), F32), dma((12,)), dma((12,)), dma((3,)), dma((3,))]
    return pl.pallas_call(
        functools.partial(_qkv_kernel, layer, gather_tab, windowed, shards),
        name=f"qkv_{layer}",
        out_shape=out_shape,
        in_specs=[vmem, vmem, hbm, hbm, hbm] + [vmem] * gather_tab,
        out_specs=[hbm] * 3 + [vmem] if gather_tab else [hbm] * 2,
        scratch_shapes=[
            *(count_scratch if gather_tab else []),
            pltpu.VMEM((4, 2 * rows, model), BF16),
            pltpu.VMEM(tab_shape, F32),
            pltpu.VMEM((model, hd), BF16),
            pltpu.VMEM((model, hd), BF16),
            pltpu.VMEM((shard, hd), BF16),
            pltpu.VMEM((held, shard, hd), BF16),
            pltpu.SemaphoreType.DMA((12,)),
            pltpu.SemaphoreType.DMA((12,)),
            pltpu.SemaphoreType.DMA((12,)),
            pltpu.SemaphoreType.DMA((12,)),
            pltpu.SemaphoreType.DMA((24,)),
            pltpu.SemaphoreType.DMA((24,)),
            pltpu.SemaphoreType.DMA((4,)),
            pltpu.SemaphoreType.DMA((4,)),
            pltpu.SemaphoreType.DMA((4,)),
            pltpu.SemaphoreType.DMA((1,)),
            pltpu.SemaphoreType.DMA((4,)),
        ],
        compiler_params=_params(4 + layer),
    )(x, gain, tab, w_q, w_kv, *([counts] if gather_tab else []))


def _attend_kernel(scale, k_block, window, marks, q_ref, kv_ref, o_ref, m_sc, l_sc, acc_sc):
    i = pl.program_id(0)
    rows, hd = q_ref.shape
    m_sc[...] = jnp.full(m_sc.shape, -1e30, F32)
    l_sc[...] = jnp.zeros(l_sc.shape, F32)
    acc_sc[...] = jnp.zeros(acc_sc.shape, F32)
    second, third, shift = marks[0], marks[1], marks[3]
    token = marks[2] + i * rows
    first = token - shift

    def lowest(t):
        low = jnp.where(t >= third, third, jnp.where(t >= second, second, 0))
        if window:
            low = jnp.maximum(low, t - (window - 1))
        return low - shift

    b_lo = lowest(token) // k_block
    b_hi = (first + rows - 1) // k_block + 1
    b_a = jnp.clip((lowest(token + rows - 1) + k_block - 1) // k_block, b_lo, b_hi)
    b_b = jnp.clip((first + 1) // k_block, b_a, b_hi)

    def block(masked, b, carry):
        start = pl.multiple_of(b * k_block, k_block)
        k = kv_ref[0, pl.ds(start, k_block), :]
        v = kv_ref[1, pl.ds(start, k_block), :]
        s = lax.dot_general(k, q_ref[...], (((1,), (1,)), ((), ())), preferred_element_type=F32)
        if masked:
            j = start + lax.broadcasted_iota(jnp.int32, (k_block, rows), 0)
            r = first + lax.broadcasted_iota(jnp.int32, (k_block, rows), 1)
            low = lowest(token + lax.broadcasted_iota(jnp.int32, (1, rows), 1))
            s = jnp.where((j <= r) & (j >= low), s, -1e30)
        m_old = m_sc[...]
        m_new = jnp.maximum(m_old, jnp.max(s, axis=0, keepdims=True))
        p = jnp.exp2((s - m_new) * scale)
        alpha = jnp.exp2((m_old - m_new) * scale)
        m_sc[...] = m_new
        l_sc[...] = l_sc[...] * alpha + jnp.sum(p, axis=0, keepdims=True)
        add = lax.dot_general(v, p.astype(BF16), (((0,), (0,)), ((), ())), preferred_element_type=F32)
        acc_sc[...] = acc_sc[...] * alpha + add
        return carry

    lax.fori_loop(b_lo, b_a, functools.partial(block, True), 0)
    lax.fori_loop(b_a, b_b, functools.partial(block, False), 0)
    lax.fori_loop(b_b, b_hi, functools.partial(block, True), 0)
    o_ref[...] = jnp.transpose(acc_sc[...] / l_sc[...]).astype(BF16)


def _attend(q, kv, marks, window, block):
    total, hd = q.shape
    blocks = total // block
    return pl.pallas_call(
        functools.partial(_attend_kernel, hd ** -0.5 * math.log2(math.e), block, window),
        name="attend",
        out_shape=jax.ShapeDtypeStruct((total, hd), BF16),
        grid_spec=pltpu.PrefetchScalarGridSpec(
            num_scalar_prefetch=1,
            grid=(blocks,),
            in_specs=[
                pl.BlockSpec((block, hd), lambda i, b: (i, 0)),
                pl.BlockSpec(memory_space=pltpu.VMEM),
            ],
            out_specs=pl.BlockSpec((block, hd), lambda i, b: (i, 0)),
            scratch_shapes=[pltpu.VMEM((1, block), F32), pltpu.VMEM((1, block), F32), pltpu.VMEM((hd, block), F32)],
        ),
        compiler_params=pltpu.CompilerParams(dimension_semantics=("arbitrary",), vmem_limit_bytes=VMEM_LIMIT),
    )(marks, q, kv)


def solution(mesh):
    tp_size, shards = mesh.shape["tp"], mesh.shape["sp"]
    row_spec = P(("dp", "sp", "tp"), None)
    id_spec = P(("dp", "sp", "tp"))
    whole = P()
    in_specs = (row_spec, id_spec, id_spec, whole, P(None, None, "tp", None), whole, whole, P(None, "tp", None, None), whole, P(None, None, "tp"), P(None, None, "tp"), P(None, "tp", None))

    def local_fn(x, segment_ids, positions, g_attn, w_q, w_k, w_v, w_o, g_mlp, w_gate, w_up, w_down):
        sp_idx = lax.axis_index("sp")
        tp_idx = lax.axis_index("tp")
        layers, model, heads_loc, hd = w_q.shape
        rows = x.shape[0]
        shard = rows * tp_size
        kv_head = tp_idx * w_k.shape[2] // tp_size
        inv_freq = ROPE_BASE ** (-jnp.arange(hd // 2, dtype=F32) / (hd // 2))
        angles = positions.astype(F32)[:, None] * inv_freq[None, :]
        tab = jnp.concatenate([jnp.cos(angles), jnp.sin(angles)], axis=1)
        counts = segment_ids.reshape(2, rows // 2)


        def pick(w):
            return lax.optimization_barrier(lax.dynamic_slice_in_dim(w, kv_head, 1, 2)).reshape(layers, model, hd)

        w_kv = lax.cond(tp_idx % 2 == 0, lambda: pick(w_k), lambda: pick(w_v))
        w_q2 = w_q.reshape(layers, model, hd)
        w_o2 = w_o.reshape(layers, hd, model)
        for layer in range(layers):
            windowed = layer % 2 == 0
            got = _qkv(layer, windowed, shards, x, g_attn, tab, w_q2, w_kv, counts)
            q, kv = got[0], got[1]
            if layer == 0:
                tab = got[2]
                tally = got[3]
                second, third = jnp.sum(tally[0:2]), jnp.sum(tally[2:4])
            q_token = sp_idx * shard
            kv_token = q_token - shard if windowed else 0
            marks = jnp.stack([second.astype(jnp.int32), third.astype(jnp.int32), q_token, kv_token]).astype(jnp.int32)
            mixed = _attend(q, kv, marks, WINDOW if windowed else 0, 512 if windowed else 1024)
            x = _block(layer, mixed, x, g_mlp, w_o2, w_gate, w_up, w_down)
        return x

    return jax.shard_map(local_fn, mesh=mesh, in_specs=in_specs, out_specs=row_spec, check_vma=False)
```
